32 devices in a mesh: dp: 4 (over x, core), wide: 8 (over z, y).
Axes of the slice: x: 2, y: 2, z: 4, core: 2. Of those that a mesh axis runs over, the one named last changes fastest.
Arguments:
- streams: float32 [4, 4096, 2048], P(None, 'dp', 'wide'), may hold values from -8 to 8
- cotangent: float32 [4, 4096, 2048], P(None, 'dp', 'wide'), may hold values from -6 to 6
- w_query: bfloat16 [2048, 2048], P('dp', 'wide'), may hold values from -2 to 2
- w_key: bfloat16 [2048, 2048], P('dp', 'wide'), may hold values from -0.125 to 0.125
- w_value: bfloat16 [2048, 2048], P('dp', 'wide'), may hold values from -0.125 to 0.125
- w_out: bfloat16 [2048, 2048], P('wide', 'dp'), may hold values from -1 to 1
- w_gate: bfloat16 [2048, 8192], P('dp', 'wide'), may hold values from -0.125 to 0.125
- w_up: bfloat16 [2048, 8192], P('dp', 'wide'), may hold values from -0.125 to 0.125
- w_down: bfloat16 [8192, 2048], P('wide', 'dp'), may hold values from -0.0625 to 0.0625
- hyper: float32 [2, 4, 6], replicated, may hold values from 0.1 to 0.6
- doc_ids: int32 [4, 1024], P('dp'), may hold values from 0 to 3, never falling along the last dimension, each value on 1 to 512 neighbouring positions
- span_starts: int32 [4, 2], P('dp'), may hold values from 0 to 768, as said below
- span_lengths: int32 [4, 2], P('dp'), may hold values from 64 to 256
Outputs:
- out_streams: float32 [4, 4096, 2048], P(None, 'dp', 'wide')
- d_streams: float32 [4, 4096, 2048], P(None, 'dp', 'wide')
- grad_query: float32 [2048, 2048], P('dp', 'wide')
- grad_key: float32 [2048, 2048], P('dp', 'wide')
- grad_value: float32 [2048, 2048], P('dp', 'wide')
- grad_out: float32 [2048, 2048], P('wide', 'dp')
- grad_gate: float32 [2048, 8192], P('dp', 'wide')
- grad_up: float32 [2048, 8192], P('dp', 'wide')
- grad_down: float32 [8192, 2048], P('wide', 'dp')
- grad_hyper: float32 [2, 4, 6], replicated
- clip_scale: float32 [16], P('wide')
- query_clipped: float32 [2048, 2048], P('dp', 'wide')
- key_clipped: float32 [2048, 2048], P('dp', 'wide')
The draws below stay inside these ranges and needn't reach their ends.
Inputs may be any that keep to these rules, and one draw needn't show every extreme that they name: `doc_ids`: each row's document numbers never fall; every document holds 1 to 512 tokens, and one holds exactly 512. `span_starts`: span k of a sequence starts and ends inside the k-th of 2 equal regions of the sequence.
All inputs are finite; a program needn't handle non-finite values.
Results may differ from the reference program's by a relative error of at most 0.018.
Values may be sent and summed in bfloat16 or wider, within the bound.
A program may use at most 192 MiB of HBM per device.

```python
import math
import jax
import jax.numpy as jnp
import numpy as np
from jax import lax

D = 2048
H = 16
FF = 8192
HEAD = 128
STREAMS = 4
LEN = 1024
SPANS = 2
SPAN_MAX = 256
DOCS = 4
CLIP_TAU = 6
SEQS = 4
TOKENS = 4096


LOG_SPREAD = 1.0986123


def draw_streams(key, part):
    noise_key = jax.random.fold_in(key, 101)
    common_key = jax.random.fold_in(key, 102)
    shape_full = (STREAMS, TOKENS, D)
    noise_part = jnp.clip(jax.random.normal(noise_key, shape_full, jnp.float32), -4.0, 4.0)
    common = jnp.clip(jax.random.normal(common_key, (STREAMS, 1, D), jnp.float32), -4.0, 4.0)
    levels = 0.8 * (jnp.arange(TOKENS, dtype=jnp.int32) // LEN).astype(jnp.float32) / max(TOKENS // LEN - 1, 1)
    return noise_part + levels[None, :, None] * common


def draw_w_query(key, part):
    base_key = jax.random.fold_in(key, 201)
    factor_key = jax.random.fold_in(key, 202)
    base_part = jnp.clip(jax.random.normal(base_key, (D, D), jnp.float32), -4.0, 4.0)
    ranks = jax.random.permutation(factor_key, jnp.arange(H, dtype=jnp.int32))
    factors = jnp.exp(LOG_SPREAD * ranks.astype(jnp.float32) / max(H - 1, 1))
    return (base_part * D ** (-0.5) * jnp.repeat(factors, D // H)[None, :]).astype(jnp.bfloat16)


def draw_span_starts(key, part):
    region = LEN // SPANS
    offsets = jax.random.randint(jax.random.fold_in(key, 301), (SEQS, SPANS), 0, region - SPAN_MAX + 1, dtype=jnp.int32)
    offsets = offsets.at[0, 0].set(0).at[0, SPANS - 1].set(region - SPAN_MAX)
    return (jnp.arange(SPANS, dtype=jnp.int32)[None, :] * region + offsets).astype(jnp.int32)


def draw_span_lengths(key, part):
    lengths = jax.random.randint(jax.random.fold_in(key, 401), (SEQS, SPANS), SPAN_MAX // 4, SPAN_MAX + 1, dtype=jnp.int32)
    return lengths.at[0, 0].set(SPAN_MAX).at[0, 1].set(SPAN_MAX // 4).astype(jnp.int32)


def level_of(stream_key, shape, pieces, smallest, top_value):
    gain = 1.0
    for dim, shards_of in pieces:
        steps = jax.random.uniform(jax.random.fold_in(jax.random.fold_in(stream_key, 6), dim), (shards_of,), jnp.float32, smallest / len(pieces), top_value / len(pieces))
        gain = gain * jnp.repeat(jnp.exp(steps), shape[dim] // shards_of).reshape((-1,) + (1,) * (len(shape) - 1 - dim))
    return gain


def profile(amount, total, most, slope):
    weights = [(1 << 20) // math.isqrt(rank ** slope) + 1 for rank in range(2, amount + 1)]
    rest, holding = total - most - (amount - 1), [1] * (amount - 1)
    while rest > 0:
        candidates = [i for i in range(amount - 1) if holding[i] < most]
        pool, remaining = sum([weights[i] for i in candidates]), rest
        for i in candidates:
            addition = min(most - holding[i], max(1, remaining * weights[i] // pool), rest)
            holding[i] = holding[i] + addition
            rest = rest - addition
    return np.array([most] + holding)


def ragged_sizes(key, number_of, total, most, slope):
    if number_of == 2:
        one = jax.random.randint(key, (), max(1, total - most), min(most, total - 1) + 1)
        return jnp.stack([one, total - one])
    sizes = jnp.asarray(profile(number_of, total, most, slope), jnp.int32)
    pairs = (number_of - 1) // 2
    source_of, sink = sizes[1:1 + 2 * pairs:2], sizes[2:2 + 2 * pairs:2]
    room = jnp.minimum(source_of - 1, most - sink)
    moved = jax.random.randint(jax.random.fold_in(key, 1), (pairs,), 0, 1 << 20) % (room + 1)
    sizes = sizes.at[1:1 + 2 * pairs:2].set(source_of - moved).at[2:2 + 2 * pairs:2].set(sink + moved)
    return sizes[jax.random.permutation(jax.random.fold_in(key, 2), number_of)]


def gaussian(stream_key, dims, scale, bound, shards=(), kind=jnp.bfloat16):
    drawn = jax.random.normal(stream_key, dims, jnp.float32) * scale
    if len(shards) > 0:
        drawn = level_of(stream_key, dims, shards, -0.22, 0.18) * drawn
    return jnp.clip(drawn, min=-bound, max=bound).astype(kind)


def setup_inputs(seed: int = 0) -> dict:
    arg_keys = jax.random.split(jax.random.key(seed), 14)
    return {
        "streams": draw_streams(jax.random.fold_in(arg_keys[13], 71), 0),
        "cotangent": gaussian(arg_keys[1], (STREAMS, TOKENS, D), 1.0, 6.0, ((1, 4), (2, 8)), jnp.float32),
        "w_query": draw_w_query(jax.random.fold_in(arg_keys[13], 71), 0),
        "w_key": gaussian(arg_keys[3], (D, D), D ** -0.5, 0.125, ((0, 4), (1, 8))),
        "w_value": gaussian(arg_keys[4], (D, D), D ** -0.5, 0.125, ((0, 4), (1, 8))),
        "w_out": gaussian(arg_keys[5], (D, D), (D // 64) ** -0.5, 1.0, ((0, 8), (1, 4))),
        "w_gate": gaussian(arg_keys[6], (D, FF), D ** -0.5, 0.125, ((0, 4), (1, 8))),
        "w_up": gaussian(arg_keys[7], (D, FF), D ** -0.5, 0.125, ((0, 4), (1, 8))),
        "w_down": gaussian(arg_keys[8], (FF, D), FF ** -0.5, 0.0625, ((0, 8), (1, 4))),
        "hyper": jnp.clip(jax.random.uniform(arg_keys[9], (2, STREAMS, STREAMS + 2), jnp.float32, 0.1, 0.6), 0.1, 0.6),
        "doc_ids": jax.vmap(lambda own: jnp.searchsorted(jnp.cumsum(ragged_sizes(own, DOCS, LEN, LEN // 2, 1)), jnp.arange(LEN), side="right"))(jax.random.split(arg_keys[10], SEQS)).reshape((SEQS, LEN)).astype(jnp.int32),
        "span_starts": draw_span_starts(jax.random.fold_in(arg_keys[13], 71), 0),
        "span_lengths": draw_span_lengths(jax.random.fold_in(arg_keys[13], 71), 0),
    }


@jax.custom_vjp
def low(v):
    return lax.optimization_barrier(v.astype(jnp.bfloat16)).astype(jnp.float32)

@jax.custom_vjp
def low_back(v):
    return v

def low_keep(v):
    return (low(v), None)

def low_pass(kept, grad):
    return (grad,)

def back_keep(v):
    return (v, None)

def back_low(kept, grad):
    return (low(grad),)
low.defvjp(low_keep, low_pass)
low_back.defvjp(back_keep, back_low)
EPSILON = 1e-05
MASKED = -1e+30
HIGHEST = lax.Precision.HIGHEST

def product(left, right):
    return jnp.dot(left, right, precision=HIGHEST, preferred_element_type=jnp.float32)

def mix_inputs(weights_in, stream_set):
    return lax.optimization_barrier(jnp.sum(weights_in[:, None, None] * stream_set, axis=0))

def mix_streams(matrix, stream_set):
    return lax.optimization_barrier(jnp.sum(matrix[:, :, None, None] * stream_set[None, :, :, :], axis=1))

def layer_norm(hidden):
    centre = lax.optimization_barrier(jnp.mean(hidden, axis=1, keepdims=True))
    centred = hidden - centre
    spread = lax.optimization_barrier(jnp.mean(centred * centred, axis=1, keepdims=True))
    return centred * lax.rsqrt(spread + EPSILON)

def rope_tables(length, head_size):
    half_size = head_size // 2
    inverse = 10000.0 ** (-2.0 * jnp.arange(half_size, dtype=jnp.float32) / head_size)
    angles = jnp.arange(length, dtype=jnp.float32)[:, None] * inverse[None, :]
    cosine_table = jnp.cos(angles)
    sine_table = jnp.sin(angles)
    return (jnp.concatenate([cosine_table, cosine_table], axis=1), jnp.concatenate([sine_table, sine_table], axis=1))

def rotate(values, cosine_table, sine_table):
    half_size = values.shape[-1] // 2
    turned = jnp.concatenate([-values[..., half_size:], values[..., :half_size]], axis=-1)
    return values * cosine_table[:, None, :] + turned * sine_table[:, None, :]

def span_labels(positions, starts, lengths):
    inside = (positions[:, None] >= starts[None, :]) & (positions[:, None] < (starts + lengths)[None, :])
    numbers = jnp.arange(1, starts.shape[0] + 1, dtype=jnp.int32)
    return lax.optimization_barrier(jnp.sum(jnp.where(inside, numbers[None, :], 0), axis=1))

def visibility(doc_row, starts, lengths):
    positions = jnp.arange(doc_row.shape[0], dtype=jnp.int32)
    labels = span_labels(positions, starts, lengths)
    same_doc = doc_row[:, None] == doc_row[None, :]
    causal = positions[None, :] <= positions[:, None]
    joint_span = (labels[:, None] > 0) & (labels[:, None] == labels[None, :])
    return same_doc & (causal | joint_span)

def sequence_layer(stream_set, weight_set, hyper_set, doc_row, starts, lengths):
    w_query, w_key, w_value, w_out, w_gate, w_up, w_down = weight_set
    length = stream_set.shape[1]
    shape_heads = (length, H, HEAD)
    cosine_table, sine_table = rope_tables(length, HEAD)
    score_scale = 1.0 / math.sqrt(HEAD)
    allowed = visibility(doc_row, starts, lengths)
    normed_one = low(layer_norm(mix_inputs(hyper_set[0, :, 0], stream_set)))
    query_raw = low_back(product(normed_one, w_query)).reshape(shape_heads)
    key_raw = low_back(product(normed_one, w_key)).reshape(shape_heads)
    values = low(low_back(product(normed_one, w_value))).reshape(shape_heads)
    queries = low(rotate(query_raw, cosine_table, sine_table))
    keys_roped = low(rotate(key_raw, cosine_table, sine_table))
    scores = low_back(jnp.einsum('qhd,khd->hqk', queries, keys_roped, precision=HIGHEST) * score_scale)
    masked = jnp.where(allowed[None, :, :], scores, MASKED)
    largest = lax.optimization_barrier(jnp.max(masked, axis=2, keepdims=True))
    exponent = jnp.exp(masked - largest)
    attention = low(exponent / lax.optimization_barrier(jnp.sum(exponent, axis=2, keepdims=True)))
    head_top = lax.optimization_barrier(jnp.max(largest, axis=(1, 2)))
    attended = jnp.einsum('hqk,khd->qhd', attention, values, precision=HIGHEST).reshape(length, H * HEAD)
    attended = low(low_back(attended))
    branch_one = low_back(product(attended, w_out))
    after_attn = mix_streams(hyper_set[0, :, 2:], stream_set) + hyper_set[0, :, 1][:, None, None] * branch_one[None, :, :]
    normed_two = low(layer_norm(mix_inputs(hyper_set[1, :, 0], after_attn)))
    gate_proj = low_back(product(normed_two, w_gate))
    up_proj = low_back(product(normed_two, w_up))
    hidden = low(gate_proj * jax.nn.sigmoid(gate_proj) * up_proj)
    branch_two = low_back(product(hidden, w_down))
    final_streams = mix_streams(hyper_set[1, :, 2:], after_attn) + hyper_set[1, :, 1][:, None, None] * branch_two[None, :, :]
    return (final_streams, head_top)

def reference(streams, cotangent, w_query, w_key, w_value, w_out, w_gate, w_up, w_down, hyper, doc_ids, span_starts, span_lengths):
    weights = tuple((matrix.astype(jnp.float32) for matrix in (w_query, w_key, w_value, w_out, w_gate, w_up, w_down)))
    count_seq = TOKENS // LEN

    def forward(stream_input, weight_set, hyper_set):
        blocks = stream_input.reshape(STREAMS, count_seq, LEN, D).transpose(1, 0, 2, 3)

        def one_sequence(inputs):
            return sequence_layer(inputs[0], weight_set, hyper_set, inputs[1], inputs[2], inputs[3])
        finals, head_tops = lax.map(jax.checkpoint(one_sequence), (blocks, doc_ids, span_starts, span_lengths))
        return (finals.transpose(1, 0, 2, 3).reshape(STREAMS, TOKENS, D), lax.optimization_barrier(jnp.max(head_tops, axis=0)))
    output, pullback, head_top = jax.vjp(forward, streams, weights, hyper.astype(jnp.float32), has_aux=True)
    stream_grad, weight_grads, hyper_grad = pullback(cotangent)
    clip_scale = jnp.sqrt(CLIP_TAU / jnp.maximum(head_top, CLIP_TAU))
    columns = jnp.repeat(clip_scale, HEAD)[None, :]
    return (output, stream_grad, weight_grads[0], weight_grads[1], weight_grads[2], weight_grads[3], weight_grads[4], weight_grads[5], weight_grads[6], hyper_grad, clip_scale, weights[0] * columns, weights[1] * columns)
```

```python
import math
from functools import partial

import jax
import jax.numpy as jnp
from jax import lax
from jax.sharding import PartitionSpec as P
from jax.experimental import pallas as pl
from jax.experimental.pallas import tpu as pltpu

D = 2048
H = 16
CLIP_TAU = 6


EPSILON = 1e-05
MASKED = -1e30

BF = jnp.bfloat16
F32 = jnp.float32
NZ = 4
def place(count):
    w = lax.axis_index("wide")
    rows_y = count // NZ
    return w, w // rows_y, w % rows_y


def greet(w, count):
    sem = pltpu.get_barrier_semaphore()
    for k in range(1, count):
        pl.semaphore_signal(sem, 1, device_id={"wide": (w + k) % count})
    pl.semaphore_wait(sem, count - 1)


def remote(src, dst, send, recv, target):
    return pltpu.make_async_remote_copy(src, dst, send, recv, device_id={"wide": target})


def dma(*shape):
    return pltpu.SemaphoreType.DMA(shape)


class Gather:
    def __init__(self, pos, count, chunks, x_ref, g_ref, sems):
        self.w, self.z, self.y = pos
        self.count, self.ny = count, count // NZ
        self.chunks, self.rows = chunks, g_ref.shape[0] // chunks
        self.x_ref, self.g_ref, self.bw = x_ref, g_ref, x_ref.shape[1]
        self.up_s, self.dn_s, self.y_s, self.z_r, self.y_r = sems

    @staticmethod
    def scratch(count, chunks):
        ny = count // NZ
        return [
            dma(NZ, chunks),
            dma(NZ, chunks),
            dma(NZ, ny - 1, chunks),
            dma(NZ, chunks),
            dma(NZ, ny - 1, chunks),
        ]

    def block(self, b, c):
        return self.g_ref.at[
            pl.ds(c * self.rows, self.rows), pl.ds(pl.multiple_of(b * self.bw, self.bw), self.bw)
        ]

    def source(self, b, c, own):
        if own:
            return self.x_ref.at[pl.ds(c * self.rows, self.rows)]
        return self.block(b, c)

    def up(self, s, zs, c):
        b = zs * self.ny + self.y
        target = (self.z + 1) * self.ny + self.y
        return remote(
            self.source(b, c, s == 0), self.block(b, c), self.up_s.at[s, c], self.z_r.at[zs, c], target
        )

    def down(self, s, zs, c):
        b = zs * self.ny + self.y
        target = (self.z - 1) * self.ny + self.y
        return remote(
            self.source(b, c, s == 0), self.block(b, c), self.dn_s.at[s, c], self.z_r.at[zs, c], target
        )

    def side(self, s, zs, k, c):
        b = zs * self.ny + self.y
        target = self.z * self.ny + (self.y + k) % self.ny
        return remote(
            self.source(b, c, s == 0),
            self.block(b, c),
            self.y_s.at[zs, k - 1, c],
            self.y_r.at[zs, k - 1, c],
            target,
        )

    def got(self, zs, c):
        b = zs * self.ny + self.y
        remote(self.block(b, c), self.block(b, c), self.up_s.at[0, c], self.z_r.at[zs, c], self.w).wait_recv()

    def got_side(self, zs):
        for k in range(1, self.ny):
            b = zs * self.ny + (self.y + self.ny - k) % self.ny
            for c in range(self.chunks):
                remote(
                    self.block(b, c),
                    self.block(b, c),
                    self.y_s.at[zs, k - 1, c],
                    self.y_r.at[zs, k - 1, c],
                    self.w,
                ).wait_recv()

    def begin(self, c):
        @pl.when(self.z < NZ - 1)
        def _():
            self.up(0, self.z, c).start()

        @pl.when(self.z > 0)
        def _():
            self.down(0, self.z, c).start()

        for k in range(1, self.ny):
            self.side(0, self.z, k, c).start()

    def place_own(self):
        self.g_ref[:, pl.ds(pl.multiple_of(self.w * self.bw, self.bw), self.bw)] = self.x_ref[...]

    def step(self, s):
        for c in range(self.chunks):

            @pl.when(self.z - s >= 0)
            def _():
                self.got(self.z - s, c)

                @pl.when(self.z < NZ - 1)
                def _():
                    self.up(s, self.z - s, c).start()

                for k in range(1, self.ny):
                    self.side(s, self.z - s, k, c).start()

            @pl.when(self.z + s < NZ)
            def _():
                self.got(self.z + s, c)

                @pl.when(self.z > 0)
                def _():
                    self.down(s, self.z + s, c).start()

                for k in range(1, self.ny):
                    self.side(s, self.z + s, k, c).start()

    def drain(self):
        for c in range(self.chunks):
            for s in range(NZ):

                @pl.when((self.z - s >= 0) & (self.z < NZ - 1))
                def _():
                    self.up(s, self.z - s, c).wait_send()

                @pl.when((self.z + s < NZ) & (self.z > 0))
                def _():
                    self.down(s, self.z + s, c).wait_send()

            for k in range(1, self.ny):
                self.side(0, self.z, k, c).wait_send()
            for s in range(1, NZ):
                for k in range(1, self.ny):

                    @pl.when(self.z - s >= 0)
                    def _():
                        self.side(s, self.z - s, k, c).wait_send()

                    @pl.when(self.z + s < NZ)
                    def _():
                        self.side(s, self.z + s, k, c).wait_send()

    def rest(self):
        for s in range(1, NZ):
            self.step(s)
        for zs in range(NZ):
            self.got_side(zs)


class Scatter:
    def __init__(self, pos, count, chunks, part, o_ref, scratch):
        self.w, self.z, self.y = pos
        self.count, self.ny = count, count // NZ
        self.chunks, self.rows = chunks, o_ref.shape[0] // chunks
        self.part, self.o_ref = part, o_ref
        (
            self.acc,
            self.ysnd,
            self.yrcv,
            self.usnd,
            self.urcv,
            self.dsnd,
            self.drcv,
            self.y_s,
            self.y_r,
            self.u_s,
            self.u_r,
            self.d_s,
            self.d_r,
        ) = scratch

    @staticmethod
    def scratch(count, chunks, tokens, bw):
        ny = count // NZ
        v = pltpu.VMEM
        rows = tokens // chunks
        return [
            v((rows, bw), F32),
            v((NZ, ny - 1, tokens, bw), BF),
            v((NZ, ny - 1, tokens, bw), BF),
            v((NZ, tokens, bw), BF),
            v((NZ, tokens, bw), BF),
            v((NZ, tokens, bw), BF),
            v((NZ, tokens, bw), BF),
            dma(NZ, ny - 1, chunks),
            dma(NZ, ny - 1, chunks),
            dma(NZ, chunks),
            dma(NZ, chunks),
            dma(NZ, chunks),
            dma(NZ, chunks),
        ]

    def order(self):
        half = self.z // (NZ // 2)
        plain = [3, 0, 2, 1]
        return [q + half * (NZ - 1 - 2 * q) for q in plain]

    def span(self, c):
        return pl.ds(c * self.rows, self.rows)

    def side(self, zd, k, c):
        rows = self.span(c)
        return remote(
            self.ysnd.at[zd, k - 1, rows],
            self.yrcv.at[zd, k - 1, rows],
            self.y_s.at[zd, k - 1, c],
            self.y_r.at[zd, k - 1, c],
            self.z * self.ny + (self.y + k) % self.ny,
        )

    def up(self, zd, c):
        rows = self.span(c)
        return remote(
            self.usnd.at[zd, rows],
            self.urcv.at[zd, rows],
            self.u_s.at[zd, c],
            self.u_r.at[zd, c],
            (self.z + 1) * self.ny + self.y,
        )

    def down(self, zd, c):
        rows = self.span(c)
        return remote(
            self.dsnd.at[zd, rows],
            self.drcv.at[zd, rows],
            self.d_s.at[zd, c],
            self.d_r.at[zd, c],
            (self.z - 1) * self.ny + self.y,
        )

    def begin(self, c):
        rows = self.span(c)
        for zd in self.order():
            for k in range(1, self.ny):
                block = zd * self.ny + (self.y + k) % self.ny
                self.ysnd[zd, k - 1, rows] = self.part(rows, block).astype(BF)
                self.side(zd, k, c).start()

    def relay(self, c):
        rows = self.span(c)
        for zd in self.order():
            value = self.part(rows, zd * self.ny + self.y)
            for k in range(1, self.ny):
                self.side(zd, k, c).wait_recv()
                value = value + self.yrcv[zd, k - 1, rows].astype(F32)
            self.acc[...] = value

            @pl.when(zd > self.z)
            def _():
                @pl.when(self.z > 0)
                def _():
                    self.up(zd, c).wait_recv()
                    self.acc[...] += self.urcv[zd, rows].astype(F32)

                self.usnd[zd, rows] = self.acc[...].astype(BF)
                self.up(zd, c).start()

            @pl.when(zd < self.z)
            def _():
                @pl.when(self.z < NZ - 1)
                def _():
                    self.down(zd, c).wait_recv()
                    self.acc[...] += self.drcv[zd, rows].astype(F32)

                self.dsnd[zd, rows] = self.acc[...].astype(BF)
                self.down(zd, c).start()

            @pl.when(zd == self.z)
            def _():
                self.o_ref[rows, :] = self.acc[...]

    def finish(self, c):
        rows = self.span(c)

        @pl.when(self.z > 0)
        def _():
            self.up(self.z, c).wait_recv()
            self.o_ref[rows, :] += self.urcv[self.z, rows].astype(F32)

        @pl.when(self.z < NZ - 1)
        def _():
            self.down(self.z, c).wait_recv()
            self.o_ref[rows, :] += self.drcv[self.z, rows].astype(F32)

    def drain(self):
        for c in range(self.chunks):
            for zd in range(NZ):
                for k in range(1, self.ny):
                    self.side(zd, k, c).wait_send()

                @pl.when(zd > self.z)
                def _():
                    self.up(zd, c).wait_send()

                @pl.when(zd < self.z)
                def _():
                    self.down(zd, c).wait_send()

    def run(self):
        self.begin(0)
        for c in range(self.chunks):
            if c + 1 < self.chunks:
                self.begin(c + 1)
            self.relay(c)
        for c in range(self.chunks):
            self.finish(c)


class Totals:
    def __init__(self, pos, count, own, buf, send, recv):
        self.w, self.count = pos[0], count
        self.own, self.buf, self.send, self.recv = own, buf, send, recv

    @staticmethod
    def scratch(count, tokens):
        return [
            pltpu.VMEM((8, tokens), F32),
            pltpu.VMEM((count, 8, tokens), F32),
            dma(count - 1),
            dma(count - 1),
        ]

    def copy(self, k):
        return remote(
            self.own, self.buf.at[k], self.send.at[k - 1], self.recv.at[k - 1], (self.w + k) % self.count
        )

    def exchange(self, first, second):
        rows = first.shape[0]
        lane = lax.broadcasted_iota(jnp.int32, (rows, 128), 1)
        pair = jnp.where(
            lane == 0, jnp.broadcast_to(first, (rows, 128)), jnp.broadcast_to(second, (rows, 128))
        )
        own = jnp.transpose(pair)[:8]
        self.own[...] = own
        for k in range(1, self.count):
            self.copy(k).start()
        total = own
        for k in range(1, self.count):
            self.copy(k).wait_recv()
            total = total + self.buf[k]
        for k in range(1, self.count):
            self.copy(k).wait_send()
        return total[0:1], total[1:2]


def column(row):
    return jnp.transpose(jnp.broadcast_to(row, (128, row.shape[1])))


def tile_columns(block, bw):
    return jnp.concatenate([block] * (bw // 128), axis=1)


def gather_kernel(count, chunks, x_ref, g_ref, *sems):
    pos = place(count)
    greet(pos[0], count)
    gather = Gather(pos, count, chunks, x_ref, g_ref, sems)
    for c in range(chunks):
        gather.begin(c)
    gather.place_own()
    gather.rest()
    gather.drain()


def norm_kernel(count, chunks, h_ref, g_ref, n_ref, i_ref, x_ref, own, buf, t_s, t_r, *sems):
    pos = place(count)
    greet(pos[0], count)
    bw = h_ref.shape[1]
    width = count * bw
    hidden = h_ref[...]
    totals = Totals(pos, count, own, buf, t_s, t_r)
    row_total, squares = totals.exchange(
        jnp.sum(hidden, axis=1, keepdims=True), jnp.sum(hidden * hidden, axis=1, keepdims=True)
    )
    centre = row_total / width
    inverse = lax.rsqrt(squares / width - centre * centre + EPSILON)
    inverse_cols = column(inverse)
    i_ref[...] = inverse_cols
    normed = (h_ref[...] - tile_columns(column(centre), bw)) * tile_columns(inverse_cols, bw)
    n_ref[...] = normed
    x_ref[...] = normed.astype(BF)
    gather = Gather(pos, count, chunks, x_ref, g_ref, sems)
    for c in range(chunks):
        gather.begin(c)
    gather.place_own()
    gather.rest()
    gather.drain()


def scatter_kernel(count, chunks, p_ref, o_ref, *scratch):
    pos = place(count)
    greet(pos[0], count)

    def part(rows, block):
        bw = p_ref.shape[1] // count
        return p_ref[rows, pl.ds(pl.multiple_of(block * bw, bw), bw)].astype(F32)

    scatter = Scatter(pos, count, chunks, part, o_ref, scratch)
    scatter.run()
    scatter.drain()


def scatter_norm_kernel(count, chunks, p_ref, n_ref, i_ref, o_ref, sum_ref, own, buf, t_s, t_r, *scratch):
    pos = place(count)
    greet(pos[0], count)
    bw = n_ref.shape[1]
    width = count * bw

    def part(rows, block):
        bw = p_ref.shape[1] // count
        return p_ref[rows, pl.ds(pl.multiple_of(block * bw, bw), bw)].astype(F32)

    scatter = Scatter(pos, count, chunks, part, sum_ref, scratch)
    scatter.run()
    grads, normed = sum_ref[...], n_ref[...]
    totals = Totals(pos, count, own, buf, t_s, t_r)
    row_total, cross = totals.exchange(
        jnp.sum(grads, axis=1, keepdims=True), jnp.sum(grads * normed, axis=1, keepdims=True)
    )
    o_ref[...] = tile_columns(i_ref[...], bw) * (
        sum_ref[...]
        - tile_columns(column(row_total / width), bw)
        - n_ref[...] * tile_columns(column(cross / width), bw)
    )
    scatter.drain()


VM = pl.BlockSpec(memory_space=pltpu.VMEM)


def call(kernel, ident, outs, ins, scratch, name, cost=None):
    return pl.pallas_call(
        kernel,
        out_shape=outs,
        in_specs=[VM] * len(ins),
        out_specs=tuple(VM for _ in outs) if isinstance(outs, tuple) else VM,
        scratch_shapes=scratch,
        compiler_params=pltpu.CompilerParams(
            collective_id=ident, has_side_effects=True, vmem_limit_bytes=60 * 1024 * 1024
        ),
        name=name,
        cost_estimate=cost or pl.CostEstimate(flops=40_000_000_000, bytes_accessed=8_000_000, transcendentals=0),
    )(*ins)


AG_CHUNKS = 8
RS_CHUNKS = 4


def features(piece, ident):
    tokens, bw = piece.shape
    count = lax.axis_size("wide")
    return call(
        partial(gather_kernel, count, AG_CHUNKS),
        ident,
        jax.ShapeDtypeStruct((tokens, count * bw), BF),
        [piece],
        Gather.scratch(count, AG_CHUNKS),
        "wide_gather",
    )


def branch_rows(partial_value, ident):
    tokens = partial_value.shape[0]
    count = lax.axis_size("wide")
    bw = partial_value.shape[1] // count
    return call(
        partial(scatter_kernel, count, RS_CHUNKS),
        ident,
        jax.ShapeDtypeStruct((tokens, bw), F32),
        [partial_value],
        Scatter.scratch(count, RS_CHUNKS, tokens, bw),
        "wide_scatter",
    )


def norm_forward(hidden, ident):
    tokens, bw = hidden.shape
    count = lax.axis_size("wide")
    return call(
        partial(norm_kernel, count, AG_CHUNKS),
        ident,
        (
            jax.ShapeDtypeStruct((tokens, count * bw), BF),
            jax.ShapeDtypeStruct((tokens, bw), F32),
            jax.ShapeDtypeStruct((tokens, 128), F32),
        ),
        [hidden],
        [pltpu.VMEM((tokens, bw), BF)] + Totals.scratch(count, tokens) + Gather.scratch(count, AG_CHUNKS),
        "norm_gather",
    )


def norm_backward(partial_value, normed, inverse, ident):
    tokens = partial_value.shape[0]
    count = lax.axis_size("wide")
    bw = partial_value.shape[1] // count
    return call(
        partial(scatter_norm_kernel, count, RS_CHUNKS),
        ident,
        jax.ShapeDtypeStruct((tokens, bw), F32),
        [partial_value, normed, inverse],
        [pltpu.VMEM((tokens, bw), F32)] + Totals.scratch(count, tokens) + Scatter.scratch(count, RS_CHUNKS, tokens, bw),
        "scatter_norm",
    )


def weight_shard(value, axis):
    return lax.psum_scatter(value.astype(BF), "dp", scatter_dimension=axis, tiled=True).astype(F32)


def rope_tables(length, head_size):
    half_size = head_size // 2
    inverse = 10000.0 ** (-2.0 * jnp.arange(half_size, dtype=jnp.float32) / head_size)
    angles = jnp.arange(length, dtype=jnp.float32)[:, None] * inverse[None, :]
    cosine_table = jnp.cos(angles)
    sine_table = jnp.sin(angles)
    return (
        jnp.concatenate([cosine_table, cosine_table], axis=1),
        jnp.concatenate([sine_table, sine_table], axis=1),
    )


def rotate(values, cosine_table, sine_table):
    half_size = values.shape[-1] // 2
    turned = jnp.concatenate([-values[..., half_size:], values[..., :half_size]], axis=-1)
    return values * cosine_table[:, None, :] + turned * sine_table[:, None, :]


def rotate_back(grads, cosine_table, sine_table):
    half_size = grads.shape[-1] // 2
    scaled = grads * sine_table[:, None, :]
    turned = jnp.concatenate([scaled[..., half_size:], -scaled[..., :half_size]], axis=-1)
    return grads * cosine_table[:, None, :] + turned


def mix_inputs(weights_in, stream_set):
    return jnp.sum(weights_in[:, None, None] * stream_set, axis=0)


def mix_streams(matrix, stream_set):
    return jnp.sum(matrix[:, :, None, None] * stream_set[None, :, :, :], axis=1)


def mix_back(matrix, grads):
    return jnp.sum(matrix[:, :, None, None] * grads[:, None, :, :], axis=0)


def hyper_rows(pre_grad, post_grad, mix_grad):
    return jnp.concatenate([pre_grad[:, None], post_grad[:, None], mix_grad], axis=1)


def span_labels(positions, starts, lengths):
    inside = (positions[:, None] >= starts[None, :]) & (
        positions[:, None] < (starts + lengths)[None, :]
    )
    numbers = jnp.arange(1, starts.shape[0] + 1, dtype=jnp.int32)
    return jnp.sum(jnp.where(inside, numbers[None, :], 0), axis=1)


def block_mask(doc_row, labels, start_row, count_rows):
    key_pos = jnp.arange(doc_row.shape[0], dtype=jnp.int32)
    query_pos = start_row + jnp.arange(count_rows, dtype=jnp.int32)
    query_docs = lax.dynamic_slice_in_dim(doc_row, start_row, count_rows)
    query_labels = lax.dynamic_slice_in_dim(labels, start_row, count_rows)
    same_doc = query_docs[:, None] == doc_row[None, :]
    causal = key_pos[None, :] <= query_pos[:, None]
    joint_span = (query_labels[:, None] > 0) & (query_labels[:, None] == labels[None, :])
    return same_doc & (causal | joint_span)


def attend_forward(queries, keys_roped, values, doc_row, starts, lengths, score_scale):
    length, head_count, head_size = queries.shape
    block_rows = min(512, length)
    labels = span_labels(jnp.arange(length, dtype=jnp.int32), starts, lengths)

    def one_block(block_index):
        start_row = block_index * block_rows
        query_rows = lax.dynamic_slice_in_dim(queries, start_row, block_rows, 0)
        scores = (
            jnp.einsum("qhd,khd->hqk", query_rows, keys_roped, preferred_element_type=jnp.float32)
            * score_scale
        )
        allowed = block_mask(doc_row, labels, start_row, block_rows)
        masked = jnp.where(allowed[None, :, :], scores, MASKED)
        largest = jnp.max(masked, axis=2)
        exponent = jnp.exp(masked - largest[:, :, None])
        totals = jnp.sum(exponent, axis=2)
        weights_low = (exponent / totals[:, :, None]).astype(jnp.bfloat16)
        attended = jnp.einsum(
            "hqk,khd->qhd", weights_low, values, preferred_element_type=jnp.float32
        )
        return (attended, largest + jnp.log(totals), jnp.max(largest, axis=1))

    attended, log_sums, block_tops = lax.map(
        one_block, jnp.arange(length // block_rows, dtype=jnp.int32)
    )
    return (attended.reshape(length, head_count, head_size), log_sums, jnp.max(block_tops, axis=0))


def attend_backward(
    queries, keys_roped, values, dout, log_sums, doc_row, starts, lengths, score_scale
):
    length, head_count, head_size = queries.shape
    block_rows = min(512, length)
    labels = span_labels(jnp.arange(length, dtype=jnp.int32), starts, lengths)

    def one_block(carry, inputs):
        key_grad, value_grad = carry
        block_index, log_rows = inputs
        start_row = block_index * block_rows
        query_rows = lax.dynamic_slice_in_dim(queries, start_row, block_rows, 0)
        dout_rows = lax.dynamic_slice_in_dim(dout, start_row, block_rows, 0)
        scores = (
            jnp.einsum("qhd,khd->hqk", query_rows, keys_roped, preferred_element_type=jnp.float32)
            * score_scale
        )
        allowed = block_mask(doc_row, labels, start_row, block_rows)
        masked = jnp.where(allowed[None, :, :], scores, MASKED)
        weights_full = jnp.where(allowed[None, :, :], jnp.exp(masked - log_rows[:, :, None]), 0.0)
        weight_grad = jnp.einsum(
            "qhd,khd->hqk", dout_rows, values, preferred_element_type=jnp.float32
        )
        centre = jnp.sum(weights_full * weight_grad, axis=2, keepdims=True)
        score_grad = (weights_full * (weight_grad - centre)).astype(jnp.bfloat16)
        query_grad = score_scale * jnp.einsum(
            "hqk,khd->qhd", score_grad, keys_roped, preferred_element_type=jnp.float32
        )
        key_grad = key_grad + score_scale * jnp.einsum(
            "hqk,qhd->khd", score_grad, query_rows, preferred_element_type=jnp.float32
        )
        value_grad = value_grad + jnp.einsum(
            "hqk,qhd->khd",
            weights_full.astype(jnp.bfloat16),
            dout_rows,
            preferred_element_type=jnp.float32,
        )
        return ((key_grad, value_grad), query_grad)

    empty_grad = jnp.zeros((length, head_count, head_size), jnp.float32)
    count_blocks = length // block_rows
    (key_grad, value_grad), query_grad = lax.scan(
        one_block, (empty_grad, empty_grad), (jnp.arange(count_blocks, dtype=jnp.int32), log_sums)
    )
    return (query_grad.reshape(length, head_count, head_size), key_grad, value_grad)


def per_device(
    streams,
    cotangent,
    w_query,
    w_key,
    w_value,
    w_out,
    w_gate,
    w_up,
    w_down,
    hyper,
    doc_ids,
    span_starts,
    span_lengths,
):
    seq_count, length = doc_ids.shape
    tokens = streams.shape[1]
    head_size = D // H
    column_count = w_query.shape[1]
    head_count = column_count // head_size
    score_scale = 1.0 / math.sqrt(head_size)
    cosine_table, sine_table = rope_tables(length, head_size)
    shape_heads = (seq_count, length, head_count, head_size)
    attn_pre, attn_post, attn_mix = (hyper[0, :, 0], hyper[0, :, 1], hyper[0, :, 2:])
    ffn_pre, ffn_post, ffn_mix = (hyper[1, :, 0], hyper[1, :, 1], hyper[1, :, 2:])
    query_w, key_w, value_w, out_w = (
        lax.all_gather(w_query, "dp", axis=0, tiled=True),
        lax.all_gather(w_key, "dp", axis=0, tiled=True),
        lax.all_gather(w_value, "dp", axis=0, tiled=True),
        lax.all_gather(w_out, "dp", axis=1, tiled=True),
    )
    gate_w, up_w, down_w = (
        lax.all_gather(w_gate, "dp", axis=0, tiled=True),
        lax.all_gather(w_up, "dp", axis=0, tiled=True),
        lax.all_gather(w_down, "dp", axis=1, tiled=True),
    )
    normed_one, kept_one, inverse_one = norm_forward(mix_inputs(attn_pre, streams), 0)
    query_raw = jnp.dot(normed_one, query_w, preferred_element_type=jnp.float32).reshape(
        shape_heads
    )
    key_raw = jnp.dot(normed_one, key_w, preferred_element_type=jnp.float32).reshape(shape_heads)
    values = (
        jnp.dot(normed_one, value_w, preferred_element_type=jnp.float32)
        .astype(jnp.bfloat16)
        .reshape(shape_heads)
    )
    queries = rotate(query_raw, cosine_table, sine_table).astype(jnp.bfloat16)
    keys_roped = rotate(key_raw, cosine_table, sine_table).astype(jnp.bfloat16)

    def forward_sequence(inputs):
        return attend_forward(
            inputs[0], inputs[1], inputs[2], inputs[3], inputs[4], inputs[5], score_scale
        )

    attended, log_sums, seq_tops = lax.map(
        forward_sequence, (queries, keys_roped, values, doc_ids, span_starts, span_lengths)
    )
    head_top = lax.pmax(jnp.max(seq_tops, axis=0), "dp")
    attended_low = attended.reshape(tokens, column_count).astype(jnp.bfloat16)
    branch_one = branch_rows(jnp.dot(attended_low, out_w, preferred_element_type=jnp.float32).astype(BF), 1)
    after_attn = mix_streams(attn_mix, streams) + attn_post[:, None, None] * branch_one[None, :, :]
    normed_two, kept_two, inverse_two = norm_forward(mix_inputs(ffn_pre, after_attn), 2)
    gate_proj = jnp.dot(normed_two, gate_w, preferred_element_type=jnp.float32)
    up_proj = jnp.dot(normed_two, up_w, preferred_element_type=jnp.float32)
    sigmoid_gate = jax.nn.sigmoid(gate_proj)
    hidden = (gate_proj * sigmoid_gate * up_proj).astype(jnp.bfloat16)
    branch_two = branch_rows(jnp.dot(hidden, down_w, preferred_element_type=jnp.float32).astype(BF), 3)
    out_streams = (
        mix_streams(ffn_mix, after_attn) + ffn_post[:, None, None] * branch_two[None, :, :]
    )
    ffn_post_grad = jnp.sum(cotangent * branch_two[None, :, :], axis=(1, 2))
    ffn_mix_grad = jnp.sum(cotangent[:, None, :, :] * after_attn[None, :, :, :], axis=(2, 3))
    two_grad = features(jnp.sum(ffn_post[:, None, None] * cotangent, axis=0).astype(BF), 4)
    hidden_grad = jnp.dot(two_grad, down_w.T, preferred_element_type=jnp.float32)
    down_wgrad = jnp.einsum("tf,td->fd", hidden, two_grad, preferred_element_type=jnp.float32)
    gate_grad = (
        hidden_grad * up_proj * sigmoid_gate * (1.0 + gate_proj * (1.0 - sigmoid_gate))
    ).astype(jnp.bfloat16)
    up_grad = (hidden_grad * gate_proj * sigmoid_gate).astype(jnp.bfloat16)
    gate_wgrad = jnp.einsum("td,tf->df", normed_two, gate_grad, preferred_element_type=jnp.float32)
    up_wgrad = jnp.einsum("td,tf->df", normed_two, up_grad, preferred_element_type=jnp.float32)
    gate_shard, up_shard, down_shard = (
        weight_shard(gate_wgrad, 0),
        weight_shard(up_wgrad, 0),
        weight_shard(down_wgrad, 1),
    )
    normed_two_grad = jnp.dot(gate_grad, gate_w.T, preferred_element_type=jnp.float32) + jnp.dot(
        up_grad, up_w.T, preferred_element_type=jnp.float32
    )
    h_two_grad = norm_backward(normed_two_grad.astype(BF), kept_two, inverse_two, 5)
    ffn_pre_grad = jnp.sum(h_two_grad[None, :, :] * after_attn, axis=(1, 2))
    after_grad = mix_back(ffn_mix, cotangent) + ffn_pre[:, None, None] * h_two_grad[None, :, :]
    attn_post_grad = jnp.sum(after_grad * branch_one[None, :, :], axis=(1, 2))
    attn_mix_grad = jnp.sum(after_grad[:, None, :, :] * streams[None, :, :, :], axis=(2, 3))
    one_grad = features(jnp.sum(attn_post[:, None, None] * after_grad, axis=0).astype(BF), 6)
    attended_grad = jnp.dot(one_grad, out_w.T, preferred_element_type=jnp.float32).astype(
        jnp.bfloat16
    )
    out_wgrad = jnp.einsum("tc,td->cd", attended_low, one_grad, preferred_element_type=jnp.float32)

    def backward_sequence(inputs):
        return attend_backward(
            inputs[0],
            inputs[1],
            inputs[2],
            inputs[3],
            inputs[4],
            inputs[5],
            inputs[6],
            inputs[7],
            score_scale,
        )

    query_grad, key_grad, value_grad = lax.map(
        backward_sequence,
        (
            queries,
            keys_roped,
            values,
            attended_grad.reshape(shape_heads),
            log_sums,
            doc_ids,
            span_starts,
            span_lengths,
        ),
    )
    query_low = (
        rotate_back(query_grad, cosine_table, sine_table)
        .reshape(tokens, column_count)
        .astype(jnp.bfloat16)
    )
    key_low = (
        rotate_back(key_grad, cosine_table, sine_table)
        .reshape(tokens, column_count)
        .astype(jnp.bfloat16)
    )
    value_low = value_grad.reshape(tokens, column_count).astype(jnp.bfloat16)
    query_wgrad = jnp.einsum("td,tc->dc", normed_one, query_low, preferred_element_type=jnp.float32)
    key_wgrad = jnp.einsum("td,tc->dc", normed_one, key_low, preferred_element_type=jnp.float32)
    value_wgrad = jnp.einsum("td,tc->dc", normed_one, value_low, preferred_element_type=jnp.float32)
    normed_one_grad = (
        jnp.dot(query_low, query_w.T, preferred_element_type=jnp.float32)
        + jnp.dot(key_low, key_w.T, preferred_element_type=jnp.float32)
        + jnp.dot(value_low, value_w.T, preferred_element_type=jnp.float32)
    )
    h_one_grad = norm_backward(normed_one_grad.astype(BF), kept_one, inverse_one, 7)
    attn_pre_grad = jnp.sum(h_one_grad[None, :, :] * streams, axis=(1, 2))
    streams_grad = mix_back(attn_mix, after_grad) + attn_pre[:, None, None] * h_one_grad[None, :, :]
    hyper_grad = lax.psum(
        jnp.stack(
            [
                hyper_rows(attn_pre_grad, attn_post_grad, attn_mix_grad),
                hyper_rows(ffn_pre_grad, ffn_post_grad, ffn_mix_grad),
            ]
        ),
        ("dp", "wide"),
    )
    query_shard, key_shard, value_shard, out_shard = (
        weight_shard(query_wgrad, 0),
        weight_shard(key_wgrad, 0),
        weight_shard(value_wgrad, 0),
        weight_shard(out_wgrad, 1),
    )
    clip_scale = jnp.sqrt(CLIP_TAU / jnp.maximum(head_top, CLIP_TAU))
    columns = jnp.repeat(clip_scale, head_size)[None, :]
    return (
        out_streams,
        streams_grad,
        query_shard,
        key_shard,
        value_shard,
        out_shard,
        gate_shard,
        up_shard,
        down_shard,
        hyper_grad,
        clip_scale,
        w_query.astype(jnp.float32) * columns,
        w_key.astype(jnp.float32) * columns,
    )


def solution(mesh):
    return jax.shard_map(
        per_device,
        mesh=mesh,
        in_specs=(
            P(None, "dp", "wide"),
            P(None, "dp", "wide"),
            P("dp", "wide"),
            P("dp", "wide"),
            P("dp", "wide"),
            P("wide", "dp"),
            P("dp", "wide"),
            P("dp", "wide"),
            P("wide", "dp"),
            P(),
            P("dp", None),
            P("dp", None),
            P("dp", None),
        ),
        out_specs=(
            P(None, "dp", "wide"),
            P(None, "dp", "wide"),
            P("dp", "wide"),
            P("dp", "wide"),
            P("dp", "wide"),
            P("wide", "dp"),
            P("dp", "wide"),
            P("dp", "wide"),
            P("wide", "dp"),
            P(),
            P("wide"),
            P("dp", "wide"),
            P("dp", "wide"),
        ),
        check_vma=False,
    )
```

```python
import math
from functools import partial

import jax
import jax.numpy as jnp
from jax import lax
from jax.sharding import PartitionSpec as P
from jax.experimental import pallas as pl
from jax.experimental.pallas import tpu as pltpu

D = 2048
H = 16
CLIP_TAU = 6


EPSILON = 1e-05
MASKED = -1e30

BF = jnp.bfloat16
F32 = jnp.float32
NZ = 4
def place(count):
    w = lax.axis_index("wide")
    rows_y = count // NZ
    return w, w // rows_y, w % rows_y


def greet(w, count, spread=None):
    sem = pltpu.get_barrier_semaphore()
    for k in range(1, count):
        pl.semaphore_signal(sem, 1, device_id={"wide": (w + k) % count})
    more = spread.greet(sem) if spread else 0
    pl.semaphore_wait(sem, count - 1 + more)


def remote(src, dst, send, recv, target):
    return pltpu.make_async_remote_copy(src, dst, send, recv, device_id={"wide": target})


def dma(*shape):
    return pltpu.SemaphoreType.DMA(shape)


class Gather:
    def __init__(self, pos, count, chunks, x_ref, g_ref, sems):
        self.w, self.z, self.y = pos
        self.count, self.ny = count, count // NZ
        self.chunks, self.rows = chunks, g_ref.shape[0] // chunks
        self.x_ref, self.g_ref, self.bw = x_ref, g_ref, x_ref.shape[1]
        self.up_s, self.dn_s, self.y_s, self.z_r, self.y_r = sems

    @staticmethod
    def scratch(count, chunks):
        ny = count // NZ
        return [
            dma(NZ, chunks),
            dma(NZ, chunks),
            dma(NZ, ny - 1, chunks),
            dma(NZ, chunks),
            dma(NZ, ny - 1, chunks),
        ]

    def block(self, b, c):
        return self.g_ref.at[
            pl.ds(c * self.rows, self.rows), pl.ds(pl.multiple_of(b * self.bw, self.bw), self.bw)
        ]

    def source(self, b, c, own):
        if own:
            return self.x_ref.at[pl.ds(c * self.rows, self.rows)]
        return self.block(b, c)

    def up(self, s, zs, c):
        b = zs * self.ny + self.y
        target = (self.z + 1) * self.ny + self.y
        return remote(
            self.source(b, c, s == 0), self.block(b, c), self.up_s.at[s, c], self.z_r.at[zs, c], target
        )

    def down(self, s, zs, c):
        b = zs * self.ny + self.y
        target = (self.z - 1) * self.ny + self.y
        return remote(
            self.source(b, c, s == 0), self.block(b, c), self.dn_s.at[s, c], self.z_r.at[zs, c], target
        )

    def side(self, s, zs, k, c):
        b = zs * self.ny + self.y
        target = self.z * self.ny + (self.y + k) % self.ny
        return remote(
            self.source(b, c, s == 0),
            self.block(b, c),
            self.y_s.at[zs, k - 1, c],
            self.y_r.at[zs, k - 1, c],
            target,
        )

    def got(self, zs, c):
        b = zs * self.ny + self.y
        remote(self.block(b, c), self.block(b, c), self.up_s.at[0, c], self.z_r.at[zs, c], self.w).wait_recv()

    def got_side(self, zs):
        for k in range(1, self.ny):
            b = zs * self.ny + (self.y + self.ny - k) % self.ny
            for c in range(self.chunks):
                remote(
                    self.block(b, c),
                    self.block(b, c),
                    self.y_s.at[zs, k - 1, c],
                    self.y_r.at[zs, k - 1, c],
                    self.w,
                ).wait_recv()

    def begin(self, c):
        @pl.when(self.z < NZ - 1)
        def _():
            self.up(0, self.z, c).start()

        @pl.when(self.z > 0)
        def _():
            self.down(0, self.z, c).start()

        for k in range(1, self.ny):
            self.side(0, self.z, k, c).start()

    def place_own(self):
        self.g_ref[:, pl.ds(pl.multiple_of(self.w * self.bw, self.bw), self.bw)] = self.x_ref[...]

    def step(self, s):
        for c in range(self.chunks):

            @pl.when(self.z - s >= 0)
            def _():
                self.got(self.z - s, c)

                @pl.when(self.z < NZ - 1)
                def _():
                    self.up(s, self.z - s, c).start()

                for k in range(1, self.ny):
                    self.side(s, self.z - s, k, c).start()

            @pl.when(self.z + s < NZ)
            def _():
                self.got(self.z + s, c)

                @pl.when(self.z > 0)
                def _():
                    self.down(s, self.z + s, c).start()

                for k in range(1, self.ny):
                    self.side(s, self.z + s, k, c).start()

    def drain(self):
        for c in range(self.chunks):
            for s in range(NZ):

                @pl.when((self.z - s >= 0) & (self.z < NZ - 1))
                def _():
                    self.up(s, self.z - s, c).wait_send()

                @pl.when((self.z + s < NZ) & (self.z > 0))
                def _():
                    self.down(s, self.z + s, c).wait_send()

            for k in range(1, self.ny):
                self.side(0, self.z, k, c).wait_send()
            for s in range(1, NZ):
                for k in range(1, self.ny):

                    @pl.when(self.z - s >= 0)
                    def _():
                        self.side(s, self.z - s, k, c).wait_send()

                    @pl.when(self.z + s < NZ)
                    def _():
                        self.side(s, self.z + s, k, c).wait_send()

    def rest(self):
        for s in range(1, NZ):
            self.step(s)
        for zs in range(NZ):
            self.got_side(zs)


class Scatter:
    def __init__(self, pos, count, chunks, part, o_ref, scratch):
        self.w, self.z, self.y = pos
        self.count, self.ny = count, count // NZ
        self.chunks, self.rows = chunks, o_ref.shape[0] // chunks
        self.part, self.o_ref = part, o_ref
        (
            self.acc,
            self.ysnd,
            self.yrcv,
            self.usnd,
            self.urcv,
            self.dsnd,
            self.drcv,
            self.y_s,
            self.y_r,
            self.u_s,
            self.u_r,
            self.d_s,
            self.d_r,
        ) = scratch

    @staticmethod
    def scratch(count, chunks, tokens, bw):
        ny = count // NZ
        v = pltpu.VMEM
        rows = tokens // chunks
        return [
            v((rows, bw), F32),
            v((NZ, ny - 1, tokens, bw), BF),
            v((NZ, ny - 1, tokens, bw), BF),
            v((NZ, tokens, bw), BF),
            v((NZ, tokens, bw), BF),
            v((NZ, tokens, bw), BF),
            v((NZ, tokens, bw), BF),
            dma(NZ, ny - 1, chunks),
            dma(NZ, ny - 1, chunks),
            dma(NZ, chunks),
            dma(NZ, chunks),
            dma(NZ, chunks),
            dma(NZ, chunks),
        ]

    def order(self):
        half = self.z // (NZ // 2)
        plain = [3, 0, 2, 1]
        return [q + half * (NZ - 1 - 2 * q) for q in plain]

    def span(self, c):
        return pl.ds(pl.multiple_of(c * self.rows, self.rows), self.rows)

    def side(self, zd, k, c):
        rows = self.span(c)
        return remote(
            self.ysnd.at[zd, k - 1, rows],
            self.yrcv.at[zd, k - 1, rows],
            self.y_s.at[zd, k - 1, c],
            self.y_r.at[zd, k - 1, c],
            self.z * self.ny + (self.y + k) % self.ny,
        )

    def up(self, zd, c):
        rows = self.span(c)
        return remote(
            self.usnd.at[zd, rows],
            self.urcv.at[zd, rows],
            self.u_s.at[zd, c],
            self.u_r.at[zd, c],
            (self.z + 1) * self.ny + self.y,
        )

    def down(self, zd, c):
        rows = self.span(c)
        return remote(
            self.dsnd.at[zd, rows],
            self.drcv.at[zd, rows],
            self.d_s.at[zd, c],
            self.d_r.at[zd, c],
            (self.z - 1) * self.ny + self.y,
        )

    def begin(self, c):
        rows = self.span(c)
        for zd in self.order():
            for k in range(1, self.ny):
                block = zd * self.ny + (self.y + k) % self.ny
                self.ysnd[zd, k - 1, rows] = self.part(rows, block).astype(BF)
                self.side(zd, k, c).start()

    def relay(self, c):
        rows = self.span(c)
        for zd in self.order():
            value = self.part(rows, zd * self.ny + self.y)
            for k in range(1, self.ny):
                self.side(zd, k, c).wait_recv()
                value = value + self.yrcv[zd, k - 1, rows].astype(F32)
            self.acc[...] = value

            @pl.when(zd > self.z)
            def _():
                @pl.when(self.z > 0)
                def _():
                    self.up(zd, c).wait_recv()
                    self.acc[...] += self.urcv[zd, rows].astype(F32)

                self.usnd[zd, rows] = self.acc[...].astype(BF)
                self.up(zd, c).start()

            @pl.when(zd < self.z)
            def _():
                @pl.when(self.z < NZ - 1)
                def _():
                    self.down(zd, c).wait_recv()
                    self.acc[...] += self.drcv[zd, rows].astype(F32)

                self.dsnd[zd, rows] = self.acc[...].astype(BF)
                self.down(zd, c).start()

            @pl.when(zd == self.z)
            def _():
                self.o_ref[rows, :] = self.acc[...]

    def finish(self, c):
        rows = self.span(c)

        @pl.when(self.z > 0)
        def _():
            self.up(self.z, c).wait_recv()
            self.o_ref[rows, :] += self.urcv[self.z, rows].astype(F32)

        @pl.when(self.z < NZ - 1)
        def _():
            self.down(self.z, c).wait_recv()
            self.o_ref[rows, :] += self.drcv[self.z, rows].astype(F32)

    def drain(self):
        for c in range(self.chunks):
            for zd in range(NZ):
                for k in range(1, self.ny):
                    self.side(zd, k, c).wait_send()

                @pl.when(zd > self.z)
                def _():
                    self.up(zd, c).wait_send()

                @pl.when(zd < self.z)
                def _():
                    self.down(zd, c).wait_send()

    def run(self):
        self.begin(0)

        def body(c, carry):
            self.begin(c + 1)
            self.relay(c)
            return carry

        lax.fori_loop(0, self.chunks - 1, body, 0)
        self.relay(self.chunks - 1)
        for c in range(self.chunks):
            self.finish(c)


class Totals:
    def __init__(self, pos, count, own, buf, send, recv):
        self.w, self.count = pos[0], count
        self.own, self.buf, self.send, self.recv = own, buf, send, recv

    @staticmethod
    def scratch(count, tokens):
        return [
            pltpu.VMEM((8, tokens), F32),
            pltpu.VMEM((count, 8, tokens), F32),
            dma(count - 1),
            dma(count - 1),
        ]

    def copy(self, k):
        return remote(
            self.own, self.buf.at[k], self.send.at[k - 1], self.recv.at[k - 1], (self.w + k) % self.count
        )

    def exchange(self, first, second):
        rows = first.shape[0]
        lane = lax.broadcasted_iota(jnp.int32, (rows, 128), 1)
        pair = jnp.where(
            lane == 0, jnp.broadcast_to(first, (rows, 128)), jnp.broadcast_to(second, (rows, 128))
        )
        own = jnp.transpose(pair)[:8]
        self.own[...] = own
        for k in range(1, self.count):
            self.copy(k).start()
        total = own
        for k in range(1, self.count):
            self.copy(k).wait_recv()
            total = total + self.buf[k]
        for k in range(1, self.count):
            self.copy(k).wait_send()
        return total[0:1], total[1:2]


def column(row):
    return jnp.transpose(jnp.broadcast_to(row, (128, row.shape[1])))


class Spread:
    def __init__(self, groups, axes, shards, wholes, sems):
        self.d = lax.axis_index("dp")
        self.groups, self.chips = groups, groups // 2
        self.x, self.core = self.d // 2, self.d % 2
        self.axes, self.shards, self.wholes = axes, shards, wholes
        self.own_s, self.own_r, self.x_s, self.x_r, self.on_s, self.on_r = sems

    @staticmethod
    def scratch(groups, parts):
        chips = groups // 2
        return [
            dma(parts),
            dma(parts),
            dma(parts, chips - 1),
            dma(parts, chips - 1),
            dma(parts, chips - 1),
            dma(parts, chips - 1),
        ]

    def greet(self, sem):
        pl.semaphore_signal(sem, 1, device_id={"dp": self.x * 2 + 1 - self.core})
        for k in range(1, self.chips):
            pl.semaphore_signal(sem, 1, device_id={"dp": (self.x + k) % self.chips * 2 + self.core})
        return self.chips

    def place(self, n, d):
        shard, whole = self.shards[n], self.wholes[n]
        if self.axes[n] == 0:
            size = shard.shape[0]
            return whole.at[pl.ds(pl.multiple_of(d * size, size), size)]
        size = shard.shape[1]
        return whole.at[:, pl.ds(pl.multiple_of(d * size, size), size)]

    def copy(self, n, src, d, send, recv, target):
        return pltpu.make_async_remote_copy(src, self.place(n, d), send, recv, device_id={"dp": target})

    def other(self):
        return self.x * 2 + 1 - self.core

    def own(self, n):
        return self.copy(n, self.shards[n], self.d, self.own_s.at[n], self.own_r.at[n], self.other())

    def along(self, n, k):
        target = (self.x + k) % self.chips * 2 + self.core
        return self.copy(n, self.shards[n], self.d, self.x_s.at[n, k - 1], self.x_r.at[n, k - 1], target)

    def onward(self, n, k):
        origin = (self.x + self.chips - k) % self.chips * 2 + self.core
        return self.copy(
            n, self.place(n, origin), origin, self.on_s.at[n, k - 1], self.on_r.at[n, k - 1], self.other()
        )

    def begin(self, n):
        for k in range(1, self.chips):
            self.along(n, k).start()
        self.own(n).start()
        self.place(n, self.d)[...] = self.shards[n][...]

    def hand_over(self, n):
        for k in range(1, self.chips):
            origin = (self.x + self.chips - k) % self.chips * 2 + self.core
            self.copy(
                n, self.place(n, origin), origin, self.x_s.at[n, k - 1], self.x_r.at[n, k - 1], self.d
            ).wait_recv()
            self.onward(n, k).start()

    def finish(self, n):
        self.copy(n, self.shards[n], self.other(), self.own_s.at[n], self.own_r.at[n], self.d).wait_recv()
        for k in range(1, self.chips):
            origin = (self.x + self.chips - k) % self.chips * 2 + 1 - self.core
            self.copy(
                n, self.place(n, origin), origin, self.on_s.at[n, k - 1], self.on_r.at[n, k - 1], self.d
            ).wait_recv()
        self.own(n).wait_send()
        for k in range(1, self.chips):
            self.along(n, k).wait_send()
            self.onward(n, k).wait_send()


def tile_columns(block, bw):
    return jnp.concatenate([block] * (bw // 128), axis=1)


def rope_tables(length, head_size):
    half_size = head_size // 2
    inverse = 10000.0 ** (-2.0 * jnp.arange(half_size, dtype=jnp.float32) / head_size)
    angles = jnp.arange(length, dtype=jnp.float32)[:, None] * inverse[None, :]
    cosine_table = jnp.cos(angles)
    sine_table = jnp.sin(angles)
    return (
        jnp.concatenate([cosine_table, cosine_table], axis=1),
        jnp.concatenate([sine_table, sine_table], axis=1),
    )


def span_labels(positions, starts, lengths):
    inside = (positions[:, None] >= starts[None, :]) & (
        positions[:, None] < (starts + lengths)[None, :]
    )
    numbers = jnp.arange(1, starts.shape[0] + 1, dtype=jnp.int32)
    return jnp.sum(jnp.where(inside, numbers[None, :], 0), axis=1)


def hyper_rows(pre_grad, post_grad, mix_grad):
    return jnp.concatenate([pre_grad[:, None], post_grad[:, None], mix_grad], axis=1)


def block_columns(ref, rows, block, count):
    bw = ref.shape[1] // count
    return ref[rows, pl.ds(pl.multiple_of(block * bw, bw), bw)]


def block_rows(ref, block, count):
    bw = ref.shape[0] // count
    return ref[pl.ds(pl.multiple_of(block * bw, bw), bw), :]


def mm(left, right):
    return jnp.dot(left, right, preferred_element_type=F32)


def mm_t(left, right):
    return lax.dot_general(left, right, (((1,), (1,)), ((), ())), preferred_element_type=F32)


def t_mm(left, right):
    return lax.dot_general(left, right, (((0,), (0,)), ((), ())), preferred_element_type=F32)


def combine(values):
    total = values[0]
    for value in values[1:]:
        total = total + value
    return total


def joint(hyper_ref):
    return combine([hyper_ref[1, i, 0] * hyper_ref[0, i, 1] for i in range(4)])


def fold(product):
    rows, width = product.shape
    grouped = jnp.sum(product.reshape(rows // 8, 8, width), axis=0)
    return combine([grouped[:, k * 128 : (k + 1) * 128] for k in range(width // 128)])


def enter_kernel(hyper_ref, s_ref, c_ref, h1_ref, hs_ref, cd_ref, two_ref, sum_ref):
    s = [s_ref[k] for k in range(4)]
    c = [c_ref[k] for k in range(4)]
    h1_ref[...] = combine([hyper_ref[0, k, 0] * s[k] for k in range(4)])
    from_s = [combine([hyper_ref[1, i, 0] * hyper_ref[0, i, 2 + k] for i in range(4)]) for k in range(4)]
    hs_ref[...] = combine([from_s[k] * s[k] for k in range(4)])
    from_c = [combine([hyper_ref[0, i, 1] * hyper_ref[1, k, 2 + i] for i in range(4)]) for k in range(4)]
    cd_ref[...] = combine([from_c[k] * c[k] for k in range(4)])
    two_ref[...] = combine([hyper_ref[1, k, 1] * c[k] for k in range(4)]).astype(BF)

    @pl.when(pl.program_id(0) == 0)
    def _():
        sum_ref[...] = jnp.zeros_like(sum_ref)

    for i in range(4):
        for k in range(4):
            sum_ref[4 * i + k] += fold(c[i] * s[k])


def leave_kernel(hyper_ref, s_ref, c_ref, b1_ref, b2_ref, d2_ref, d1_ref, out_ref, grad_ref, sum_ref):
    s = [s_ref[k] for k in range(4)]
    c = [c_ref[k] for k in range(4)]
    b1, b2, d2, d1 = b1_ref[...], b2_ref[...], d2_ref[...], d1_ref[...]
    for i in range(4):
        coef = [combine([hyper_ref[1, i, 2 + j] * hyper_ref[0, j, 2 + k] for j in range(4)]) for k in range(4)]
        from_b = combine([hyper_ref[1, i, 2 + j] * hyper_ref[0, j, 1] for j in range(4)])
        out_ref[i] = combine([coef[k] * s[k] for k in range(4)]) + from_b * b1 + hyper_ref[1, i, 1] * b2
    for j in range(4):
        coef = [combine([hyper_ref[0, i, 2 + j] * hyper_ref[1, k, 2 + i] for i in range(4)]) for k in range(4)]
        from_d = combine([hyper_ref[0, i, 2 + j] * hyper_ref[1, i, 0] for i in range(4)])
        grad_ref[j] = combine([coef[k] * c[k] for k in range(4)]) + from_d * d2 + hyper_ref[0, j, 0] * d1

    @pl.when(pl.program_id(0) == 0)
    def _():
        sum_ref[...] = jnp.zeros_like(sum_ref)

    for k in range(4):
        sum_ref[k] += fold(c[k] * b1)
        sum_ref[4 + k] += fold(c[k] * b2)
        sum_ref[8 + k] += fold(d2 * s[k])
        sum_ref[12 + k] += fold(d1 * s[k])
    sum_ref[16] += fold(d2 * b1)


def total_kernel(count, groups, a_ref, b_ref, top_ref, o_ref, m_ref, own, dbuf, wbuf, mown, mbuf, ds, dr, ws, wr, ms, mr):
    w, d = lax.axis_index("wide"), lax.axis_index("dp")
    sem = pltpu.get_barrier_semaphore()
    for k in range(1, count):
        pl.semaphore_signal(sem, 1, device_id={"wide": (w + k) % count})
    for k in range(1, groups):
        pl.semaphore_signal(sem, 1, device_id={"dp": (d + k) % groups})
    pl.semaphore_wait(sem, count + groups - 2)
    na, nb = a_ref.shape[0], b_ref.shape[0]
    own[...] = jnp.zeros_like(own)
    for k in range(na):
        own[k : k + 1, :] = jnp.sum(a_ref[k], axis=0, keepdims=True)
    for k in range(nb):
        own[na + k : na + k + 1, :] = jnp.sum(b_ref[k], axis=0, keepdims=True)
    mown[...] = top_ref[...]

    def over_dp(src, dst, send, recv, k):
        return pltpu.make_async_remote_copy(
            src, dst.at[k - 1], send.at[k - 1], recv.at[k - 1], device_id={"dp": (d + k) % groups}
        )

    for k in range(1, groups):
        over_dp(own, dbuf, ds, dr, k).start()
        over_dp(mown, mbuf, ms, mr, k).start()
    total, best = own[...], mown[...]
    for k in range(1, groups):
        over_dp(own, dbuf, ds, dr, k).wait_recv()
        over_dp(mown, mbuf, ms, mr, k).wait_recv()
        total = total + dbuf[k - 1]
        best = jnp.maximum(best, mbuf[k - 1])
    m_ref[...] = best
    for k in range(1, groups):
        over_dp(own, dbuf, ds, dr, k).wait_send()
        over_dp(mown, mbuf, ms, mr, k).wait_send()
    own[...] = total

    def over_wide(k):
        return remote(own, wbuf.at[k - 1], ws.at[k - 1], wr.at[k - 1], (w + k) % count)

    for k in range(1, count):
        over_wide(k).start()
    for k in range(1, count):
        over_wide(k).wait_recv()
        total = total + wbuf[k - 1]
    for k in range(1, count):
        over_wide(k).wait_send()
    o_ref[...] = jnp.broadcast_to(jnp.sum(total, axis=1, keepdims=True), o_ref.shape)


def normalize(pos, count, hidden_ref, n_ref, i_ref, x_ref, totals):
    bw = hidden_ref.shape[1]
    width = count * bw
    hidden = hidden_ref[...]
    row_total, squares = totals.exchange(
        jnp.sum(hidden, axis=1, keepdims=True), jnp.sum(hidden * hidden, axis=1, keepdims=True)
    )
    centre = row_total / width
    inverse = lax.rsqrt(squares / width - centre * centre + EPSILON)
    inverse_cols = column(inverse)
    i_ref[...] = inverse_cols
    normed = (hidden_ref[...] - tile_columns(column(centre), bw)) * tile_columns(inverse_cols, bw)
    n_ref[...] = normed
    x_ref[...] = normed.astype(BF)


def denormalize(pos, count, sum_ref, n_ref, i_ref, o_ref, totals):
    bw = n_ref.shape[1]
    width = count * bw
    grads = sum_ref[...]
    row_total, cross = totals.exchange(
        jnp.sum(grads, axis=1, keepdims=True), jnp.sum(grads * n_ref[...], axis=1, keepdims=True)
    )
    o_ref[...] = tile_columns(i_ref[...], bw) * (
        sum_ref[...]
        - tile_columns(column(row_total / width), bw)
        - n_ref[...] * tile_columns(column(cross / width), bw)
    )


def first_kernel(count, groups, chunks, h_ref, sq, sk, sv, so, g_ref, n_ref, i_ref, wq, wk, wv, wo, x_ref, *rest):
    pos = place(count)
    spread = Spread(groups, (0, 0, 0, 1), (sq, sk, sv, so), (wq, wk, wv, wo), rest[:6])
    greet(pos[0], count, spread)
    for n in range(4):
        spread.begin(n)
    totals = Totals(pos, count, *rest[6:10])
    normalize(pos, count, h_ref, n_ref, i_ref, x_ref, totals)
    gather = Gather(pos, count, chunks, x_ref, g_ref, rest[10:])
    for c in range(chunks):
        gather.begin(c)
    gather.place_own()
    for n in range(2):
        spread.hand_over(n)
    gather.step(1)
    for n in range(2, 4):
        spread.hand_over(n)
    gather.step(2)
    gather.step(3)
    for zs in range(NZ):
        gather.got_side(zs)
    for n in range(4):
        spread.finish(n)
    gather.drain()


def head_mask(doc_rows, doc_cols, lab_rows, lab_cols, r0, c0, rows, cols):
    q = r0 + lax.broadcasted_iota(jnp.int32, (rows, cols), 0)
    k = c0 + lax.broadcasted_iota(jnp.int32, (rows, cols), 1)
    same = doc_rows == doc_cols
    joined = (lab_rows > 0) & (lab_rows == lab_cols)
    return same & ((k <= q) | joined)


QB = 256
DOC_MAX = 512
SPANS = 2


def key_range(r0, length):
    low = max(0, (r0 - DOC_MAX + 1) // QB * QB)
    region = length // SPANS
    high = min(length, (r0 // region + 1) * region)
    return low, high


def turn(values, cos, sin):
    half = values.shape[1] // 2
    turned = jnp.concatenate([-values[:, half:], values[:, :half]], axis=1)
    return values * cos + turned * sin


def turn_back(grads, cos, sin):
    half = grads.shape[1] // 2
    scaled = grads * sin
    turned = jnp.concatenate([scaled[:, half:], -scaled[:, :half]], axis=1)
    return grads * cos + turned


HD = D // H


def attention_rows(h, r0, scale, length, q_ref, k_ref, v_ref, o_ref, lse_ref, top_ref, masks):
    cols = slice(h * HD, (h + 1) * HD)
    low, high = key_range(r0, length)
    doc_c, doc_r, lab_c, lab_r = masks
    s = mm_t(q_ref[r0 : r0 + QB, cols], k_ref[low:high, cols]) * scale
    allowed = head_mask(
        doc_c[r0 : r0 + QB, :1],
        doc_r[:1, low:high],
        lab_c[r0 : r0 + QB, :1],
        lab_r[:1, low:high],
        r0,
        low,
        QB,
        high - low,
    )
    s = jnp.where(allowed, s, MASKED)
    largest = jnp.max(s, axis=1, keepdims=True)
    e = jnp.exp(s - largest)
    total = jnp.sum(e, axis=1, keepdims=True)
    weights = (e / total).astype(BF)
    o_ref[r0 : r0 + QB, cols] = mm(weights, v_ref[low:high, cols]).astype(BF)
    lse_ref[h, r0 : r0 + QB, :] = jnp.broadcast_to(largest + jnp.log(total), (QB, 128))
    top_ref[h : h + 1, :] = jnp.maximum(top_ref[h : h + 1, :], jnp.max(largest))


def attention_kernel(count, chunks, scale, x_ref, wq, wk, wv, cos_ref, sin_ref, doc_c, doc_r, lab_c, lab_r, two_ref,
                     q_ref, k_ref, v_ref, o_ref, lse_ref, top_ref, g_ref, *sems):
    pos = place(count)
    greet(pos[0], count)
    gather = Gather(pos, count, chunks, two_ref, g_ref, sems)
    for c in range(chunks):
        gather.begin(c)
    gather.place_own()
    length, width = q_ref.shape
    heads = width // HD
    top_ref[...] = jnp.full(top_ref.shape, MASKED, F32)
    v_ref[...] = mm(x_ref[...], wv[...]).astype(BF)
    for target, weight in ((q_ref, wq), (k_ref, wk)):
        for h in range(heads):
            cols = slice(h * HD, (h + 1) * HD)
            raw = mm(x_ref[...], weight[:, cols])
            target[:, cols] = turn(raw, cos_ref[...], sin_ref[...]).astype(BF)
    gather.step(1)
    masks = (doc_c, doc_r, lab_c, lab_r)
    todo = [(h, r0) for h in range(heads) for r0 in range(0, length, QB)]
    for n, (h, r0) in enumerate(todo):
        attention_rows(h, r0, scale, length, q_ref, k_ref, v_ref, o_ref, lse_ref, top_ref, masks)
        if n == len(todo) // 2 - 1:
            gather.step(2)
    gather.step(3)
    for zs in range(NZ):
        gather.got_side(zs)
    gather.drain()


def middle_kernel(count, g_chunks, s_chunks, hyper_ref, att_ref, wo_ref, hs_ref, wg_hbm, wu_hbm, wd_hbm, two_hbm,
                  b1_ref, n_ref, i_ref, x2_ref, hid_ref, dg_ref, du_ref,
                  wg, wu, wd, two, load, dhid, h_ref, x_ref, *rest):
    pos = place(count)
    loads = [
        pltpu.make_async_copy(src, dst, load.at[n])
        for n, (src, dst) in enumerate(((wd_hbm, wd), (two_hbm, two), (wg_hbm, wg), (wu_hbm, wu)))
    ]
    for copy in loads:
        copy.start()
    greet(pos[0], count)

    def part(rows, block):
        return mm(att_ref[rows, :], block_columns(wo_ref, slice(None), block, count))

    scatter = Scatter(pos, count, s_chunks, part, b1_ref, rest[:13])
    scatter.run()
    h_ref[...] = hs_ref[...] + joint(hyper_ref) * b1_ref[...]
    totals = Totals(pos, count, *rest[13:17])
    normalize(pos, count, h_ref, n_ref, i_ref, x_ref, totals)
    gather = Gather(pos, count, g_chunks, x_ref, x2_ref, rest[17:])
    for c in range(g_chunks):
        gather.begin(c)
    gather.place_own()
    tokens, width = hid_ref.shape
    tile = 256
    half = tokens // 2
    steps = width // tile

    def where(n):
        rows = pl.ds(pl.multiple_of((n // steps) * half, half), half)
        cols = pl.ds(pl.multiple_of((n % steps) * tile, tile), tile)
        return rows, cols

    def down_back(n, carry):
        rows, cols = where(n)
        dhid[rows, cols] = mm_t(two[rows, :], wd[cols, :])
        return carry

    loads[0].wait()
    loads[1].wait()
    gather.step(1)
    lax.fori_loop(0, steps, down_back, 0)
    gather.step(2)
    lax.fori_loop(steps, 2 * steps, down_back, 0)
    gather.step(3)
    for zs in range(NZ):
        gather.got_side(zs)
    loads[2].wait()
    loads[3].wait()

    def feed(n, carry):
        rows, cols = where(n)
        gate = mm(x2_ref[rows, :], wg[:, cols])
        up = mm(x2_ref[rows, :], wu[:, cols])
        sg = 1.0 / (1.0 + jnp.exp(-gate))
        back = dhid[rows, cols]
        swish = gate * sg
        hid_ref[rows, cols] = (swish * up).astype(BF)
        dg_ref[rows, cols] = (back * up * sg * (1.0 + gate * (1.0 - sg))).astype(BF)
        du_ref[rows, cols] = (back * swish).astype(BF)
        return carry

    lax.fori_loop(0, 2 * steps, feed, 0)
    scatter.drain()
    gather.drain()


def second_kernel(count, g_chunks, s_chunks, hyper_ref, dg_ref, du_ref, wg, wu, n_ref, i_ref, cd_ref,
                  d2_ref, one_ref, sum_ref, x_ref, *rest):
    pos = place(count)
    greet(pos[0], count)

    def part(rows, block):
        return mm_t(dg_ref[rows, :], block_rows(wg, block, count)) + mm_t(
            du_ref[rows, :], block_rows(wu, block, count)
        )

    scatter = Scatter(pos, count, s_chunks, part, sum_ref, rest[:13])
    scatter.run()
    totals = Totals(pos, count, *rest[13:17])
    denormalize(pos, count, sum_ref, n_ref, i_ref, d2_ref, totals)
    x_ref[...] = (cd_ref[...] + joint(hyper_ref) * d2_ref[...]).astype(BF)
    gather = Gather(pos, count, g_chunks, x_ref, one_ref, rest[17:])
    for c in range(g_chunks):
        gather.begin(c)
    gather.place_own()
    gather.rest()
    scatter.drain()
    gather.drain()


def back_rows(h, r0, scale, length, q_ref, k_ref, v_ref, do_ref, lse_ref, dq_acc, dk_acc, dv_acc, masks):
    cols = slice(h * HD, (h + 1) * HD)
    rows = slice(r0, r0 + QB)
    low, high = key_range(r0, length)
    doc_c, doc_r, lab_c, lab_r = masks
    q, k, v, do = q_ref[rows, cols], k_ref[low:high, cols], v_ref[low:high, cols], do_ref[rows, cols]
    s = mm_t(q, k) * scale
    allowed = head_mask(
        doc_c[rows, :1], doc_r[:1, low:high], lab_c[rows, :1], lab_r[:1, low:high], r0, low, QB, high - low
    )
    weights = jnp.where(allowed, jnp.exp(jnp.where(allowed, s, MASKED) - lse_ref[h, rows, :1]), 0.0)
    grad = mm_t(do, v)
    centre = jnp.sum(weights * grad, axis=1, keepdims=True)
    ds = (weights * (grad - centre)).astype(BF)
    dq_acc[rows, cols] = mm(ds, k) * scale
    dk_acc[low:high, cols] += t_mm(ds, q)
    dv_acc[low:high, cols] += t_mm(weights.astype(BF), do)


def attention_back_kernel(count, s_chunks, scale, one_ref, wo_ref, q_ref, k_ref, v_ref, lse_ref, cos_ref, sin_ref,
                          doc_c, doc_r, lab_c, lab_r, hid_ref, wd_ref,
                          dq_ref, dk_ref, dv_ref, b2_ref, do_ref, dq_acc, dk_acc, dv_acc, *scratch):
    pos = place(count)
    greet(pos[0], count)

    def part(rows, block):
        return mm(hid_ref[rows, :], block_columns(wd_ref, slice(None), block, count))

    scatter = Scatter(pos, count, s_chunks, part, b2_ref, scratch)
    scatter.begin(0)
    length, width = q_ref.shape
    heads = width // HD
    do_ref[...] = mm_t(one_ref[...], wo_ref[...]).astype(BF)
    dk_acc[...] = jnp.zeros_like(dk_acc)
    dv_acc[...] = jnp.zeros_like(dv_acc)
    masks = (doc_c, doc_r, lab_c, lab_r)
    todo = [(h, r0) for h in range(heads) for r0 in range(0, length, QB)]
    for n, (h, r0) in enumerate(todo):
        if n * s_chunks % len(todo) == 0 or s_chunks > len(todo):
            c = n * s_chunks // len(todo)
            if c + 1 < s_chunks:
                scatter.begin(c + 1)
            scatter.relay(c)
        back_rows(h, r0, scale, length, q_ref, k_ref, v_ref, do_ref, lse_ref, dq_acc, dk_acc, dv_acc, masks)
    for h in range(heads):
        cols = slice(h * HD, (h + 1) * HD)
        dq_ref[:, cols] = turn_back(dq_acc[:, cols], cos_ref[...], sin_ref[...]).astype(BF)
        dk_ref[:, cols] = turn_back(dk_acc[:, cols] * scale, cos_ref[...], sin_ref[...]).astype(BF)
    dv_ref[...] = dv_acc[...].astype(BF)
    for c in range(s_chunks):
        scatter.finish(c)
    scatter.drain()


def last_kernel(count, s_chunks, dq_ref, dk_ref, dv_ref, wq, wk, wv, n_ref, i_ref, d1_ref, sum_ref, *rest):
    pos = place(count)
    greet(pos[0], count)

    def part(rows, block):
        return (
            mm_t(dq_ref[rows, :], block_rows(wq, block, count))
            + mm_t(dk_ref[rows, :], block_rows(wk, block, count))
            + mm_t(dv_ref[rows, :], block_rows(wv, block, count))
        )

    scatter = Scatter(pos, count, s_chunks, part, sum_ref, rest[:13])
    scatter.run()
    totals = Totals(pos, count, *rest[13:])
    denormalize(pos, count, sum_ref, n_ref, i_ref, d1_ref, totals)
    scatter.drain()


VM = pl.BlockSpec(memory_space=pltpu.VMEM)
SM = pl.BlockSpec(memory_space=pltpu.SMEM)
ANY = pl.BlockSpec(memory_space=pl.ANY)


def call(kernel, ident, outs, ins, scratch, name, specs=None):
    return pl.pallas_call(
        kernel,
        out_shape=outs,
        in_specs=specs or [VM] * len(ins),
        out_specs=tuple(VM for _ in outs) if isinstance(outs, tuple) else VM,
        scratch_shapes=scratch,
        compiler_params=pltpu.CompilerParams(
            collective_id=ident, has_side_effects=True, vmem_limit_bytes=63 * 1024 * 1024
        ),
        name=name,
        cost_estimate=pl.CostEstimate(flops=50_000_000_000, bytes_accessed=8_000_000, transcendentals=0),
    )(*ins)


def shape(dtype, *dims):
    return jax.ShapeDtypeStruct(dims, dtype)


AG_CHUNKS = 8
RS_CHUNKS = 4
ROWS = 128


def rows_call(kernel, hyper, ins, outs, name):
    tokens = ins[0].shape[-2]

    def spec(a):
        if a.shape[-2] != tokens:
            return pl.BlockSpec(a.shape, lambda t: (0,) * len(a.shape))
        if len(a.shape) == 3:
            return pl.BlockSpec((a.shape[0], ROWS, a.shape[2]), lambda t: (0, t, 0))
        return pl.BlockSpec((ROWS, a.shape[1]), lambda t: (t, 0))

    return pl.pallas_call(
        kernel,
        grid=(tokens // ROWS,),
        out_shape=outs,
        in_specs=[SM] + [spec(a) for a in ins],
        out_specs=tuple(spec(a) for a in outs),
        compiler_params=pltpu.CompilerParams(vmem_limit_bytes=32 * 1024 * 1024),
        name=name,
        cost_estimate=pl.CostEstimate(flops=1_000_000_000, bytes_accessed=20_000_000, transcendentals=0),
    )(hyper, *ins)


def weight_sum(left, right):
    return lax.dot_general(left, right, (((0,), (0,)), ((), ())), preferred_element_type=F32).astype(BF)


def weight_shard(value, axis):
    return lax.psum_scatter(value, "dp", scatter_dimension=axis, tiled=True).astype(F32)


def hyper_grad(hyper, v):
    pre1, post0, mix0, mix1 = hyper[1, :, 0], hyper[0, :, 1], hyper[0, :, 2:], hyper[1, :, 2:]
    cs, cb1, cb2, d2s, d1s, d2b1 = v[:16].reshape(4, 4), v[16:20], v[20:24], v[24:28], v[28:32], v[32]
    flat = partial(jnp.sum, axis=-1)
    g1_pre = flat(mix0 * d2s[None, :]) + post0 * d2b1
    g1_mix = jnp.sum(cs[:, None, :] * mix0[None, :, :], axis=2) + cb1[:, None] * post0[None, :]
    g0_post = jnp.sum(mix1 * cb1[:, None], axis=0) + pre1 * d2b1
    g0_mix = jnp.sum(mix1[:, :, None] * cs[:, None, :], axis=0) + pre1[:, None] * d2s[None, :]
    return jnp.stack([hyper_rows(d1s, g0_post, g0_mix), hyper_rows(g1_pre, cb2, g1_mix)])


def per_device(
    streams,
    cotangent,
    w_query,
    w_key,
    w_value,
    w_out,
    w_gate,
    w_up,
    w_down,
    hyper,
    doc_ids,
    span_starts,
    span_lengths,
):
    length = doc_ids.shape[1]
    tokens, bw = streams.shape[1:]
    count, groups = lax.axis_size("wide"), lax.axis_size("dp")
    heads = bw // HD
    scale = 1.0 / math.sqrt(HD)
    cos, sin = rope_tables(length, HD)
    labels = span_labels(jnp.arange(length, dtype=jnp.int32), span_starts[0], span_lengths[0])
    doc_r = jnp.broadcast_to(doc_ids, (8, length))
    lab_r = jnp.broadcast_to(labels[None, :], (8, length))
    doc_c = jnp.broadcast_to(doc_ids[0][:, None], (length, 128))
    lab_c = jnp.broadcast_to(labels[:, None], (length, 128))
    masks = [doc_c, doc_r, lab_c, lab_r]
    gate_w, up_w, down_w = (
        lax.all_gather(w_gate, "dp", axis=0, tiled=True),
        lax.all_gather(w_up, "dp", axis=0, tiled=True),
        lax.all_gather(w_down, "dp", axis=1, tiled=True),
    )
    hidden_units = gate_w.shape[1]
    small = shape(F32, tokens, bw)
    low = shape(BF, tokens, bw)
    whole = shape(BF, tokens, count * bw)
    stat = shape(F32, tokens, 128)
    wide_low = shape(BF, tokens, hidden_units)
    v = pltpu.VMEM
    scatter_scratch = Scatter.scratch(count, RS_CHUNKS, tokens, bw)
    gather_scratch = Gather.scratch(count, AG_CHUNKS)
    total_scratch = Totals.scratch(count, tokens)

    h_one, h_streams, cot_one, two_part, sums_a = rows_call(
        enter_kernel, hyper, [streams, cotangent], (small, small, small, low, shape(F32, 16, 8, 128)), "enter"
    )
    tall = shape(BF, count * bw, bw)
    x_one, kept_one, inverse_one, query_w, key_w, value_w, out_w = call(
        partial(first_kernel, count, groups, AG_CHUNKS),
        0,
        (whole, small, stat, tall, tall, tall, shape(BF, bw, count * bw)),
        [h_one, w_query, w_key, w_value, w_out],
        [v((tokens, bw), BF)] + Spread.scratch(groups, 4) + total_scratch + gather_scratch,
        "first",
    )
    queries, keys, values, attended, log_sums, tops, two_grad = call(
        partial(attention_kernel, count, AG_CHUNKS, scale),
        1,
        (low, low, low, low, shape(F32, heads, tokens, 128), shape(F32, 8, 128), whole),
        [x_one, query_w, key_w, value_w, cos, sin] + masks + [two_part],
        gather_scratch,
        "attention",
    )
    branch_one, kept_two, inverse_two, x_two, hidden, gate_grad, up_grad = call(
        partial(middle_kernel, count, AG_CHUNKS, RS_CHUNKS),
        2,
        (small, small, stat, whole, wide_low, wide_low, wide_low),
        [hyper, attended, out_w, h_streams, gate_w, up_w, down_w, two_grad],
        [
            v(gate_w.shape, BF),
            v(up_w.shape, BF),
            v(down_w.shape, BF),
            v((tokens, count * bw), BF),
            dma(4),
            v((tokens, hidden_units), F32),
            v((tokens, bw), F32),
            v((tokens, bw), BF),
        ]
        + scatter_scratch
        + total_scratch
        + gather_scratch,
        "middle",
        [SM, VM, VM, VM, ANY, ANY, ANY, ANY],
    )
    down_sum, gate_sum, up_sum = (
        weight_sum(hidden, two_grad),
        weight_sum(x_two, gate_grad),
        weight_sum(x_two, up_grad),
    )
    gate_grad, up_grad, hidden, down_sum, gate_sum, up_sum = lax.optimization_barrier(
        (gate_grad, up_grad, hidden, down_sum, gate_sum, up_sum)
    )
    down_shard, gate_shard, up_shard = (
        weight_shard(down_sum, 1),
        weight_shard(gate_sum, 0),
        weight_shard(up_sum, 0),
    )
    h_two_grad, one_grad = call(
        partial(second_kernel, count, AG_CHUNKS, RS_CHUNKS),
        3,
        (small, whole),
        [hyper, gate_grad, up_grad, gate_w, up_w, kept_two, inverse_two, cot_one],
        [v((tokens, bw), F32), v((tokens, bw), BF)] + scatter_scratch + total_scratch + gather_scratch,
        "second",
        [SM] + [VM] * 7,
    )
    query_low, key_low, value_low, branch_two = call(
        partial(attention_back_kernel, count, RS_CHUNKS, scale),
        4,
        (low, low, low, small),
        [one_grad, out_w, queries, keys, values, log_sums, cos, sin] + masks + [hidden, down_w],
        [v((tokens, bw), BF)] + [v((tokens, bw), F32)] * 3 + scatter_scratch,
        "attention_back",
    )
    query_low, key_low, value_low, one_grad, down_shard, gate_shard, up_shard = lax.optimization_barrier(
        (query_low, key_low, value_low, one_grad, down_shard, gate_shard, up_shard)
    )
    query_low, key_low, value_low, out_sum, query_sum, key_sum, value_sum = lax.optimization_barrier(
        (
            query_low,
            key_low,
            value_low,
            weight_sum(attended, one_grad),
            weight_sum(x_one, query_low),
            weight_sum(x_one, key_low),
            weight_sum(x_one, value_low),
        )
    )
    out_shard, query_shard, key_shard, value_shard = (
        weight_shard(out_sum, 1),
        weight_shard(query_sum, 0),
        weight_shard(key_sum, 0),
        weight_shard(value_sum, 0),
    )
    h_one_grad = call(
        partial(last_kernel, count, RS_CHUNKS),
        5,
        small,
        [query_low, key_low, value_low, query_w, key_w, value_w, kept_one, inverse_one],
        [v((tokens, bw), F32)] + scatter_scratch + total_scratch,
        "last",
    )
    streams_shape = shape(F32, 4, tokens, bw)
    out_streams, streams_grad, sums_b = rows_call(
        leave_kernel,
        hyper,
        [streams, cotangent, branch_one, branch_two, h_two_grad, h_one_grad],
        (streams_shape, streams_shape, shape(F32, 17, 8, 128)),
        "leave",
    )
    sums, best = call(
        partial(total_kernel, count, groups),
        6,
        (shape(F32, 40, 128), shape(F32, 8, 128)),
        [sums_a, sums_b, tops],
        [
            v((40, 128), F32),
            v((groups - 1, 40, 128), F32),
            v((count - 1, 40, 128), F32),
            v((8, 128), F32),
            v((groups - 1, 8, 128), F32),
            dma(groups - 1),
            dma(groups - 1),
            dma(count - 1),
            dma(count - 1),
            dma(groups - 1),
            dma(groups - 1),
        ],
        "totals",
    )
    head_top = best[:heads, 0]
    clip_scale = jnp.sqrt(CLIP_TAU / jnp.maximum(head_top, CLIP_TAU))
    columns = jnp.repeat(clip_scale, HD)[None, :]
    return (
        out_streams,
        streams_grad,
        query_shard,
        key_shard,
        value_shard,
        out_shard,
        gate_shard,
        up_shard,
        down_shard,
        hyper_grad(hyper, sums[:, 0]),
        clip_scale,
        w_query.astype(F32) * columns,
        w_key.astype(F32) * columns,
    )


def solution(mesh):
    return jax.shard_map(
        per_device,
        mesh=mesh,
        in_specs=(
            P(None, "dp", "wide"),
            P(None, "dp", "wide"),
            P("dp", "wide"),
            P("dp", "wide"),
            P("dp", "wide"),
            P("wide", "dp"),
            P("dp", "wide"),
            P("dp", "wide"),
            P("wide", "dp"),
            P(),
            P("dp", None),
            P("dp", None),
            P("dp", None),
        ),
        out_specs=(
            P(None, "dp", "wide"),
            P(None, "dp", "wide"),
            P("dp", "wide"),
            P("dp", "wide"),
            P("dp", "wide"),
            P("wide", "dp"),
            P("dp", "wide"),
            P("dp", "wide"),
            P("wide", "dp"),
            P(),
            P("wide"),
            P("dp", "wide"),
            P("dp", "wide"),
        ),
        check_vma=False,
    )
```

```python
import math
from functools import partial

import jax
import jax.numpy as jnp
from jax import lax
from jax.sharding import PartitionSpec as P
from jax.experimental import pallas as pl
from jax.experimental.pallas import tpu as pltpu

D = 2048
H = 16
CLIP_TAU = 6


EPSILON = 1e-05
MASKED = -1e30

BF = jnp.bfloat16
F32 = jnp.float32
NZ = 4
def place(count):
    w = lax.axis_index("wide")
    rows_y = count // NZ
    return w, w // rows_y, w % rows_y


def greet(w, count, spread=None):
    sem = pltpu.get_barrier_semaphore()
    for k in range(1, count):
        pl.semaphore_signal(sem, 1, device_id={"wide": (w + k) % count})
    more = spread.greet(sem) if spread else 0
    pl.semaphore_wait(sem, count - 1 + more)


def remote(src, dst, send, recv, target):
    return pltpu.make_async_remote_copy(src, dst, send, recv, device_id={"wide": target})


def dma(*shape):
    return pltpu.SemaphoreType.DMA(shape)


class Gather:
    def __init__(self, pos, count, chunks, x_ref, g_ref, sems):
        self.w, self.z, self.y = pos
        self.count, self.ny = count, count // NZ
        self.chunks, self.rows = chunks, g_ref.shape[0] // chunks
        self.x_ref, self.g_ref, self.bw = x_ref, g_ref, x_ref.shape[1]
        self.up_s, self.dn_s, self.y_s, self.z_r, self.y_r = sems

    @staticmethod
    def scratch(count, chunks):
        ny = count // NZ
        return [
            dma(NZ, chunks),
            dma(NZ, chunks),
            dma(NZ, ny - 1, chunks),
            dma(NZ, chunks),
            dma(NZ, ny - 1, chunks),
        ]

    def block(self, b, c):
        return self.g_ref.at[
            pl.ds(c * self.rows, self.rows), pl.ds(pl.multiple_of(b * self.bw, self.bw), self.bw)
        ]

    def source(self, b, c, own):
        if own:
            return self.x_ref.at[pl.ds(c * self.rows, self.rows)]
        return self.block(b, c)

    def up(self, s, zs, c):
        b = zs * self.ny + self.y
        target = (self.z + 1) * self.ny + self.y
        return remote(
            self.source(b, c, s == 0), self.block(b, c), self.up_s.at[s, c], self.z_r.at[zs, c], target
        )

    def down(self, s, zs, c):
        b = zs * self.ny + self.y
        target = (self.z - 1) * self.ny + self.y
        return remote(
            self.source(b, c, s == 0), self.block(b, c), self.dn_s.at[s, c], self.z_r.at[zs, c], target
        )

    def side(self, s, zs, k, c):
        b = zs * self.ny + self.y
        target = self.z * self.ny + (self.y + k) % self.ny
        return remote(
            self.source(b, c, s == 0),
            self.block(b, c),
            self.y_s.at[zs, k - 1, c],
            self.y_r.at[zs, k - 1, c],
            target,
        )

    def got(self, zs, c):
        b = zs * self.ny + self.y
        remote(self.block(b, c), self.block(b, c), self.up_s.at[0, c], self.z_r.at[zs, c], self.w).wait_recv()

    def got_side(self, zs):
        for k in range(1, self.ny):
            b = zs * self.ny + (self.y + self.ny - k) % self.ny
            for c in range(self.chunks):
                remote(
                    self.block(b, c),
                    self.block(b, c),
                    self.y_s.at[zs, k - 1, c],
                    self.y_r.at[zs, k - 1, c],
                    self.w,
                ).wait_recv()

    def begin(self, c):
        @pl.when(self.z < NZ - 1)
        def _():
            self.up(0, self.z, c).start()

        @pl.when(self.z > 0)
        def _():
            self.down(0, self.z, c).start()

        for k in range(1, self.ny):
            self.side(0, self.z, k, c).start()

    def place_own(self):
        self.g_ref[:, pl.ds(pl.multiple_of(self.w * self.bw, self.bw), self.bw)] = self.x_ref[...]

    def step(self, s, part=0, parts=1):
        size = self.chunks // parts
        for c in range(part * size, (part + 1) * size):

            @pl.when(self.z - s >= 0)
            def _():
                self.got(self.z - s, c)

                @pl.when(self.z < NZ - 1)
                def _():
                    self.up(s, self.z - s, c).start()

                for k in range(1, self.ny):
                    self.side(s, self.z - s, k, c).start()

            @pl.when(self.z + s < NZ)
            def _():
                self.got(self.z + s, c)

                @pl.when(self.z > 0)
                def _():
                    self.down(s, self.z + s, c).start()

                for k in range(1, self.ny):
                    self.side(s, self.z + s, k, c).start()

    def drain(self):
        for c in range(self.chunks):
            for s in range(NZ):

                @pl.when((self.z - s >= 0) & (self.z < NZ - 1))
                def _():
                    self.up(s, self.z - s, c).wait_send()

                @pl.when((self.z + s < NZ) & (self.z > 0))
                def _():
                    self.down(s, self.z + s, c).wait_send()

            for k in range(1, self.ny):
                self.side(0, self.z, k, c).wait_send()
            for s in range(1, NZ):
                for k in range(1, self.ny):

                    @pl.when(self.z - s >= 0)
                    def _():
                        self.side(s, self.z - s, k, c).wait_send()

                    @pl.when(self.z + s < NZ)
                    def _():
                        self.side(s, self.z + s, k, c).wait_send()

    def rest(self):
        for s in range(1, NZ):
            self.step(s)
        for zs in range(NZ):
            self.got_side(zs)


class Scatter:
    def __init__(self, pos, count, chunks, part, o_ref, scratch):
        self.w, self.z, self.y = pos
        self.count, self.ny = count, count // NZ
        self.chunks, self.rows = chunks, o_ref.shape[0] // chunks
        self.part, self.o_ref = part, o_ref
        (
            self.acc,
            self.ysnd,
            self.yrcv,
            self.usnd,
            self.urcv,
            self.dsnd,
            self.drcv,
            self.y_s,
            self.y_r,
            self.u_s,
            self.u_r,
            self.d_s,
            self.d_r,
        ) = scratch

    @staticmethod
    def scratch(count, chunks, tokens, bw):
        ny = count // NZ
        v = pltpu.VMEM
        rows = tokens // chunks
        return [
            v((rows, bw), F32),
            v((NZ, ny - 1, tokens, bw), BF),
            v((NZ, ny - 1, tokens, bw), BF),
            v((NZ, tokens, bw), BF),
            v((NZ, tokens, bw), BF),
            v((NZ, tokens, bw), BF),
            v((NZ, tokens, bw), BF),
            dma(NZ, ny - 1, chunks),
            dma(NZ, ny - 1, chunks),
            dma(NZ, chunks),
            dma(NZ, chunks),
            dma(NZ, chunks),
            dma(NZ, chunks),
        ]

    def order(self):
        half = self.z // (NZ // 2)
        plain = [3, 0, 2, 1]
        return [q + half * (NZ - 1 - 2 * q) for q in plain]

    def span(self, c):
        return pl.ds(pl.multiple_of(c * self.rows, self.rows), self.rows)

    def side(self, zd, k, c):
        rows = self.span(c)
        return remote(
            self.ysnd.at[zd, k - 1, rows],
            self.yrcv.at[zd, k - 1, rows],
            self.y_s.at[zd, k - 1, c],
            self.y_r.at[zd, k - 1, c],
            self.z * self.ny + (self.y + k) % self.ny,
        )

    def up(self, zd, c):
        rows = self.span(c)
        return remote(
            self.usnd.at[zd, rows],
            self.urcv.at[zd, rows],
            self.u_s.at[zd, c],
            self.u_r.at[zd, c],
            (self.z + 1) * self.ny + self.y,
        )

    def down(self, zd, c):
        rows = self.span(c)
        return remote(
            self.dsnd.at[zd, rows],
            self.drcv.at[zd, rows],
            self.d_s.at[zd, c],
            self.d_r.at[zd, c],
            (self.z - 1) * self.ny + self.y,
        )

    def begin(self, c):
        rows = self.span(c)
        for zd in self.order():
            for k in range(1, self.ny):
                block = zd * self.ny + (self.y + k) % self.ny
                self.ysnd[zd, k - 1, rows] = self.part(rows, block).astype(BF)
                self.side(zd, k, c).start()

    def relay(self, c):
        rows = self.span(c)
        for zd in self.order():
            value = self.part(rows, zd * self.ny + self.y)
            for k in range(1, self.ny):
                self.side(zd, k, c).wait_recv()
                value = value + self.yrcv[zd, k - 1, rows].astype(F32)
            self.acc[...] = value

            @pl.when(zd > self.z)
            def _():
                @pl.when(self.z > 0)
                def _():
                    self.up(zd, c).wait_recv()
                    self.acc[...] += self.urcv[zd, rows].astype(F32)

                self.usnd[zd, rows] = self.acc[...].astype(BF)
                self.up(zd, c).start()

            @pl.when(zd < self.z)
            def _():
                @pl.when(self.z < NZ - 1)
                def _():
                    self.down(zd, c).wait_recv()
                    self.acc[...] += self.drcv[zd, rows].astype(F32)

                self.dsnd[zd, rows] = self.acc[...].astype(BF)
                self.down(zd, c).start()

            @pl.when(zd == self.z)
            def _():
                self.o_ref[rows, :] = self.acc[...]

    def finish(self, c):
        rows = self.span(c)

        @pl.when(self.z > 0)
        def _():
            self.up(self.z, c).wait_recv()
            self.o_ref[rows, :] += self.urcv[self.z, rows].astype(F32)

        @pl.when(self.z < NZ - 1)
        def _():
            self.down(self.z, c).wait_recv()
            self.o_ref[rows, :] += self.drcv[self.z, rows].astype(F32)

    def drain(self):
        for c in range(self.chunks):
            for zd in range(NZ):
                for k in range(1, self.ny):
                    self.side(zd, k, c).wait_send()

                @pl.when(zd > self.z)
                def _():
                    self.up(zd, c).wait_send()

                @pl.when(zd < self.z)
                def _():
                    self.down(zd, c).wait_send()

    def run(self, work=()):
        work = list(work)
        self.begin(0)
        if work:
            for c in range(self.chunks):
                if c + 1 < self.chunks:
                    self.begin(c + 1)
                for item in work[c :: self.chunks]:
                    item()
                self.relay(c)
        else:

            def body(c, carry):
                self.begin(c + 1)
                self.relay(c)
                return carry

            lax.fori_loop(0, self.chunks - 1, body, 0)
            self.relay(self.chunks - 1)
        for c in range(self.chunks):
            self.finish(c)


class Totals:
    def __init__(self, pos, count, own, buf, send, recv):
        self.w, self.count = pos[0], count
        self.own, self.buf, self.send, self.recv = own, buf, send, recv

    @staticmethod
    def scratch(count, tokens):
        return [
            pltpu.VMEM((8, tokens), F32),
            pltpu.VMEM((count, 8, tokens), F32),
            dma(count - 1),
            dma(count - 1),
        ]

    def copy(self, k):
        return remote(
            self.own, self.buf.at[k], self.send.at[k - 1], self.recv.at[k - 1], (self.w + k) % self.count
        )

    def exchange(self, first, second):
        rows = first.shape[0]
        lane = lax.broadcasted_iota(jnp.int32, (rows, 128), 1)
        pair = jnp.where(
            lane == 0, jnp.broadcast_to(first, (rows, 128)), jnp.broadcast_to(second, (rows, 128))
        )
        own = jnp.transpose(pair)[:8]
        self.own[...] = own
        for k in range(1, self.count):
            self.copy(k).start()
        total = own
        for k in range(1, self.count):
            self.copy(k).wait_recv()
            total = total + self.buf[k]
        for k in range(1, self.count):
            self.copy(k).wait_send()
        return total[0:1], total[1:2]


def column(row):
    return jnp.transpose(jnp.broadcast_to(row, (128, row.shape[1])))


class Spread:
    def __init__(self, groups, axes, shards, wholes, sems):
        self.d = lax.axis_index("dp")
        self.groups, self.chips = groups, groups // 2
        self.x, self.core = self.d // 2, self.d % 2
        self.axes, self.shards, self.wholes = axes, shards, wholes
        self.own_s, self.own_r, self.x_s, self.x_r, self.on_s, self.on_r = sems

    @staticmethod
    def scratch(groups, parts):
        chips = groups // 2
        return [
            dma(parts),
            dma(parts),
            dma(parts, chips - 1),
            dma(parts, chips - 1),
            dma(parts, chips - 1),
            dma(parts, chips - 1),
        ]

    def greet(self, sem):
        pl.semaphore_signal(sem, 1, device_id={"dp": self.x * 2 + 1 - self.core})
        for k in range(1, self.chips):
            pl.semaphore_signal(sem, 1, device_id={"dp": (self.x + k) % self.chips * 2 + self.core})
        return self.chips

    def place(self, n, d):
        shard, whole = self.shards[n], self.wholes[n]
        if self.axes[n] == 0:
            size = shard.shape[0]
            return whole.at[pl.ds(pl.multiple_of(d * size, size), size)]
        size = shard.shape[1]
        return whole.at[:, pl.ds(pl.multiple_of(d * size, size), size)]

    def copy(self, n, src, d, send, recv, target):
        return pltpu.make_async_remote_copy(src, self.place(n, d), send, recv, device_id={"dp": target})

    def other(self):
        return self.x * 2 + 1 - self.core

    def own(self, n):
        return self.copy(n, self.shards[n], self.d, self.own_s.at[n], self.own_r.at[n], self.other())

    def along(self, n, k):
        target = (self.x + k) % self.chips * 2 + self.core
        return self.copy(n, self.shards[n], self.d, self.x_s.at[n, k - 1], self.x_r.at[n, k - 1], target)

    def onward(self, n, k):
        origin = (self.x + self.chips - k) % self.chips * 2 + self.core
        return self.copy(
            n, self.place(n, origin), origin, self.on_s.at[n, k - 1], self.on_r.at[n, k - 1], self.other()
        )

    def begin(self, n):
        for k in range(1, self.chips):
            self.along(n, k).start()
        self.own(n).start()
        self.place(n, self.d)[...] = self.shards[n][...]

    def hand_over(self, n):
        for k in range(1, self.chips):
            origin = (self.x + self.chips - k) % self.chips * 2 + self.core
            self.copy(
                n, self.place(n, origin), origin, self.x_s.at[n, k - 1], self.x_r.at[n, k - 1], self.d
            ).wait_recv()
            self.onward(n, k).start()

    def finish(self, n):
        self.copy(n, self.shards[n], self.other(), self.own_s.at[n], self.own_r.at[n], self.d).wait_recv()
        for k in range(1, self.chips):
            origin = (self.x + self.chips - k) % self.chips * 2 + 1 - self.core
            self.copy(
                n, self.place(n, origin), origin, self.on_s.at[n, k - 1], self.on_r.at[n, k - 1], self.d
            ).wait_recv()
        self.own(n).wait_send()
        for k in range(1, self.chips):
            self.along(n, k).wait_send()
            self.onward(n, k).wait_send()


class Reduce:
    def __init__(self, groups, axis, lhs, rhs, outs, scratch):
        d = lax.axis_index("dp")
        self.x, self.core, self.chips = d // 2, d % 2, groups // 2
        self.axis, self.lhs, self.rhs, self.outs = axis, lhs, rhs, outs
        self.turned, self.snd, self.rcv, self.xs, self.xr, self.s_s, self.s_r, self.x_s, self.x_r = scratch
        self.rows, self.width = outs[0].shape
        self.tile = min(256, self.width)
        if axis == 1:
            self.turned[...] = jnp.transpose(lhs[...])

    @staticmethod
    def scratch(groups, axis, lhs, outs):
        chips = groups // 2
        rows, width = outs[0].shape
        v, n = pltpu.VMEM, len(outs)
        return [
            v((rows, lhs.shape[0]), BF),
            v((n, chips, rows, width), BF),
            v((n, chips, rows, width), BF),
            v((n, chips - 1, rows, width), BF),
            v((n, chips - 1, rows, width), BF),
            dma(n, chips),
            dma(n, chips),
            dma(n, chips - 1),
            dma(n, chips - 1),
        ]

    def greet(self, sem):
        pl.semaphore_signal(sem, 1, device_id={"dp": self.x * 2 + 1 - self.core})
        for k in range(1, self.chips):
            pl.semaphore_signal(sem, 1, device_id={"dp": (self.x + k) % self.chips * 2 + self.core})
        return self.chips

    def prepare(self, d):
        if self.axis == 0:
            self.turned[...] = jnp.transpose(self.lhs[:, pl.ds(pl.multiple_of(d * self.rows, self.rows), self.rows)])

    def product(self, n, d, j):
        start = j * self.tile if self.axis == 0 else d * self.width + j * self.tile
        return mm(self.turned[...], self.rhs[n][:, pl.ds(pl.multiple_of(start, self.tile), self.tile)])

    def cols(self, j):
        return pl.ds(pl.multiple_of(j * self.tile, self.tile), self.tile)

    def tiles(self, body):
        def loop(j, carry):
            body(j)
            return carry

        lax.fori_loop(0, self.width // self.tile, loop, 0)

    def across(self, n, k):
        other = self.x * 2 + 1 - self.core
        return pltpu.make_async_remote_copy(
            self.snd.at[n, k], self.rcv.at[n, k], self.s_s.at[n, k], self.s_r.at[n, k], device_id={"dp": other}
        )

    def along(self, n, k):
        target = (self.x + k) % self.chips * 2 + self.core
        return pltpu.make_async_remote_copy(
            self.xs.at[n, k - 1],
            self.xr.at[n, k - 1],
            self.x_s.at[n, k - 1],
            self.x_r.at[n, k - 1],
            device_id={"dp": target},
        )

    def give(self, k):
        d = (self.x + k) % self.chips * 2 + 1 - self.core
        self.prepare(d)
        for n in range(len(self.outs)):

            def body(j):
                self.snd[n, k, :, self.cols(j)] = self.product(n, d, j).astype(BF)

            self.tiles(body)
            self.across(n, k).start()

    def take(self, k):
        d = (self.x + k) % self.chips * 2 + self.core
        self.prepare(d)
        for n in range(len(self.outs)):
            self.across(n, k).wait_recv()

            def body(j):
                total = self.product(n, d, j) + self.rcv[n, k, :, self.cols(j)].astype(F32)
                if k == 0:
                    self.outs[n][:, self.cols(j)] = total
                else:
                    self.xs[n, k - 1, :, self.cols(j)] = total.astype(BF)

            self.tiles(body)
            if k > 0:
                self.along(n, k).start()

    def work(self):
        order = list(range(1, self.chips)) + [0]
        return [partial(self.give, k) for k in order] + [partial(self.take, k) for k in order]

    def finish(self):
        for n in range(len(self.outs)):
            for k in range(1, self.chips):
                self.along(n, k).wait_recv()

                def body(j):
                    self.outs[n][:, self.cols(j)] += self.xr[n, k - 1, :, self.cols(j)].astype(F32)

                self.tiles(body)
        for n in range(len(self.outs)):
            for k in range(self.chips):
                self.across(n, k).wait_send()
                if k > 0:
                    self.along(n, k).wait_send()


def tile_columns(block, bw):
    return jnp.concatenate([block] * (bw // 128), axis=1)


def rope_tables(length, head_size):
    half_size = head_size // 2
    inverse = 10000.0 ** (-2.0 * jnp.arange(half_size, dtype=jnp.float32) / head_size)
    angles = jnp.arange(length, dtype=jnp.float32)[:, None] * inverse[None, :]
    cosine_table = jnp.cos(angles)
    sine_table = jnp.sin(angles)
    return (
        jnp.concatenate([cosine_table, cosine_table], axis=1),
        jnp.concatenate([sine_table, sine_table], axis=1),
    )


def span_labels(positions, starts, lengths):
    inside = (positions[:, None] >= starts[None, :]) & (
        positions[:, None] < (starts + lengths)[None, :]
    )
    numbers = jnp.arange(1, starts.shape[0] + 1, dtype=jnp.int32)
    return jnp.sum(jnp.where(inside, numbers[None, :], 0), axis=1)


def hyper_rows(pre_grad, post_grad, mix_grad):
    return jnp.concatenate([pre_grad[:, None], post_grad[:, None], mix_grad], axis=1)


def block_columns(ref, rows, block, count):
    bw = ref.shape[1] // count
    return ref[rows, pl.ds(pl.multiple_of(block * bw, bw), bw)]


def block_rows(ref, block, count):
    bw = ref.shape[0] // count
    return ref[pl.ds(pl.multiple_of(block * bw, bw), bw), :]


def mm(left, right):
    return jnp.dot(left, right, preferred_element_type=F32)


def mm_t(left, right):
    return lax.dot_general(left, right, (((1,), (1,)), ((), ())), preferred_element_type=F32)


def t_mm(left, right):
    return lax.dot_general(left, right, (((0,), (0,)), ((), ())), preferred_element_type=F32)


def combine(values):
    total = values[0]
    for value in values[1:]:
        total = total + value
    return total


def joint(hyper_ref):
    return combine([hyper_ref[1, i, 0] * hyper_ref[0, i, 1] for i in range(4)])


def fold(product):
    rows, width = product.shape
    grouped = jnp.sum(product.reshape(rows // 8, 8, width), axis=0)
    return combine([grouped[:, k * 128 : (k + 1) * 128] for k in range(width // 128)])


def enter_kernel(hyper_ref, s_ref, c_ref, h1_ref, hs_ref, cd_ref, two_ref, sum_ref):
    s = [s_ref[k] for k in range(4)]
    c = [c_ref[k] for k in range(4)]
    h1_ref[...] = combine([hyper_ref[0, k, 0] * s[k] for k in range(4)])
    from_s = [combine([hyper_ref[1, i, 0] * hyper_ref[0, i, 2 + k] for i in range(4)]) for k in range(4)]
    hs_ref[...] = combine([from_s[k] * s[k] for k in range(4)])
    from_c = [combine([hyper_ref[0, i, 1] * hyper_ref[1, k, 2 + i] for i in range(4)]) for k in range(4)]
    cd_ref[...] = combine([from_c[k] * c[k] for k in range(4)])
    two_ref[...] = combine([hyper_ref[1, k, 1] * c[k] for k in range(4)]).astype(BF)

    @pl.when(pl.program_id(0) == 0)
    def _():
        sum_ref[...] = jnp.zeros_like(sum_ref)

    for i in range(4):
        for k in range(4):
            sum_ref[4 * i + k] += fold(c[i] * s[k])


def leave_kernel(hyper_ref, s_ref, c_ref, b1_ref, b2_ref, d2_ref, d1_ref, out_ref, grad_ref, sum_ref):
    s = [s_ref[k] for k in range(4)]
    c = [c_ref[k] for k in range(4)]
    b1, b2, d2, d1 = b1_ref[...], b2_ref[...], d2_ref[...], d1_ref[...]
    for i in range(4):
        coef = [combine([hyper_ref[1, i, 2 + j] * hyper_ref[0, j, 2 + k] for j in range(4)]) for k in range(4)]
        from_b = combine([hyper_ref[1, i, 2 + j] * hyper_ref[0, j, 1] for j in range(4)])
        out_ref[i] = combine([coef[k] * s[k] for k in range(4)]) + from_b * b1 + hyper_ref[1, i, 1] * b2
    for j in range(4):
        coef = [combine([hyper_ref[0, i, 2 + j] * hyper_ref[1, k, 2 + i] for i in range(4)]) for k in range(4)]
        from_d = combine([hyper_ref[0, i, 2 + j] * hyper_ref[1, i, 0] for i in range(4)])
        grad_ref[j] = combine([coef[k] * c[k] for k in range(4)]) + from_d * d2 + hyper_ref[0, j, 0] * d1

    @pl.when(pl.program_id(0) == 0)
    def _():
        sum_ref[...] = jnp.zeros_like(sum_ref)

    for k in range(4):
        sum_ref[k] += fold(c[k] * b1)
        sum_ref[4 + k] += fold(c[k] * b2)
        sum_ref[8 + k] += fold(d2 * s[k])
        sum_ref[12 + k] += fold(d1 * s[k])
    sum_ref[16] += fold(d2 * b1)


def total_kernel(count, groups, a_ref, b_ref, top_ref, o_ref, m_ref, own, dbuf, wbuf, mown, mbuf, ds, dr, ws, wr, ms, mr):
    w, d = lax.axis_index("wide"), lax.axis_index("dp")
    sem = pltpu.get_barrier_semaphore()
    for k in range(1, count):
        pl.semaphore_signal(sem, 1, device_id={"wide": (w + k) % count})
    for k in range(1, groups):
        pl.semaphore_signal(sem, 1, device_id={"dp": (d + k) % groups})
    pl.semaphore_wait(sem, count + groups - 2)
    na, nb = a_ref.shape[0], b_ref.shape[0]
    own[...] = jnp.zeros_like(own)
    for k in range(na):
        own[k : k + 1, :] = jnp.sum(a_ref[k], axis=0, keepdims=True)
    for k in range(nb):
        own[na + k : na + k + 1, :] = jnp.sum(b_ref[k], axis=0, keepdims=True)
    mown[...] = top_ref[...]

    def over_dp(src, dst, send, recv, k):
        return pltpu.make_async_remote_copy(
            src, dst.at[k - 1], send.at[k - 1], recv.at[k - 1], device_id={"dp": (d + k) % groups}
        )

    for k in range(1, groups):
        over_dp(own, dbuf, ds, dr, k).start()
        over_dp(mown, mbuf, ms, mr, k).start()
    total, best = own[...], mown[...]
    for k in range(1, groups):
        over_dp(own, dbuf, ds, dr, k).wait_recv()
        over_dp(mown, mbuf, ms, mr, k).wait_recv()
        total = total + dbuf[k - 1]
        best = jnp.maximum(best, mbuf[k - 1])
    m_ref[...] = best
    for k in range(1, groups):
        over_dp(own, dbuf, ds, dr, k).wait_send()
        over_dp(mown, mbuf, ms, mr, k).wait_send()
    own[...] = total

    def over_wide(k):
        return remote(own, wbuf.at[k - 1], ws.at[k - 1], wr.at[k - 1], (w + k) % count)

    for k in range(1, count):
        over_wide(k).start()
    for k in range(1, count):
        over_wide(k).wait_recv()
        total = total + wbuf[k - 1]
    for k in range(1, count):
        over_wide(k).wait_send()
    o_ref[...] = jnp.broadcast_to(jnp.sum(total, axis=1, keepdims=True), o_ref.shape)


def normalize(pos, count, hidden_ref, n_ref, i_ref, x_ref, totals):
    bw = hidden_ref.shape[1]
    width = count * bw
    hidden = hidden_ref[...]
    row_total, squares = totals.exchange(
        jnp.sum(hidden, axis=1, keepdims=True), jnp.sum(hidden * hidden, axis=1, keepdims=True)
    )
    centre = row_total / width
    inverse = lax.rsqrt(squares / width - centre * centre + EPSILON)
    inverse_cols = column(inverse)
    i_ref[...] = inverse_cols
    normed = (hidden_ref[...] - tile_columns(column(centre), bw)) * tile_columns(inverse_cols, bw)
    n_ref[...] = normed
    x_ref[...] = normed.astype(BF)


def denormalize(pos, count, sum_ref, n_ref, i_ref, o_ref, totals):
    bw = n_ref.shape[1]
    width = count * bw
    grads = sum_ref[...]
    row_total, cross = totals.exchange(
        jnp.sum(grads, axis=1, keepdims=True), jnp.sum(grads * n_ref[...], axis=1, keepdims=True)
    )
    o_ref[...] = tile_columns(i_ref[...], bw) * (
        sum_ref[...]
        - tile_columns(column(row_total / width), bw)
        - n_ref[...] * tile_columns(column(cross / width), bw)
    )


def first_kernel(count, groups, chunks, h_ref, sq, sk, sv, so, g_ref, n_ref, i_ref, wq, wk, wv, wo, x_ref, *rest):
    pos = place(count)
    spread = Spread(groups, (0, 0, 0, 1), (sq, sk, sv, so), (wq, wk, wv, wo), rest[:6])
    greet(pos[0], count, spread)
    for n in range(4):
        spread.begin(n)
    totals = Totals(pos, count, *rest[6:10])
    normalize(pos, count, h_ref, n_ref, i_ref, x_ref, totals)
    gather = Gather(pos, count, chunks, x_ref, g_ref, rest[10:])
    for c in range(chunks):
        gather.begin(c)
    gather.place_own()
    gather.step(1)
    gather.step(2)
    for n in range(2):
        spread.hand_over(n)
    gather.step(3)
    for n in range(2, 4):
        spread.hand_over(n)
    for zs in range(NZ):
        gather.got_side(zs)
    for n in range(4):
        spread.finish(n)
    gather.drain()


def head_mask(doc_rows, doc_cols, lab_rows, lab_cols, r0, c0, rows, cols):
    q = r0 + lax.broadcasted_iota(jnp.int32, (rows, cols), 0)
    k = c0 + lax.broadcasted_iota(jnp.int32, (rows, cols), 1)
    same = doc_rows == doc_cols
    joined = (lab_rows > 0) & (lab_rows == lab_cols)
    return same & ((k <= q) | joined)


QB = 256
DOC_MAX = 512
SPANS = 2


def key_range(r0, length):
    low = max(0, (r0 - DOC_MAX + 1) // QB * QB)
    region = length // SPANS
    high = min(length, (r0 // region + 1) * region)
    return low, high


def turn(values, cos, sin):
    half = values.shape[1] // 2
    turned = jnp.concatenate([-values[:, half:], values[:, :half]], axis=1)
    return values * cos + turned * sin


def turn_back(grads, cos, sin):
    half = grads.shape[1] // 2
    scaled = grads * sin
    turned = jnp.concatenate([scaled[:, half:], -scaled[:, :half]], axis=1)
    return grads * cos + turned


HD = D // H


def attention_rows(h, r0, scale, length, q_ref, k_ref, v_ref, o_ref, lse_ref, top_ref, masks):
    cols = slice(h * HD, (h + 1) * HD)
    low, high = key_range(r0, length)
    doc_c, doc_r, lab_c, lab_r = masks
    s = mm_t(q_ref[r0 : r0 + QB, cols], k_ref[low:high, cols]) * scale
    allowed = head_mask(
        doc_c[r0 : r0 + QB, :1],
        doc_r[:1, low:high],
        lab_c[r0 : r0 + QB, :1],
        lab_r[:1, low:high],
        r0,
        low,
        QB,
        high - low,
    )
    s = jnp.where(allowed, s, MASKED)
    largest = jnp.max(s, axis=1, keepdims=True)
    e = jnp.exp(s - largest)
    total = jnp.sum(e, axis=1, keepdims=True)
    weights = (e / total).astype(BF)
    o_ref[r0 : r0 + QB, cols] = mm(weights, v_ref[low:high, cols]).astype(BF)
    lse_ref[h, r0 : r0 + QB, :] = jnp.broadcast_to(largest + jnp.log(total), (QB, 128))
    top_ref[h : h + 1, :] = jnp.maximum(top_ref[h : h + 1, :], jnp.max(largest))


def attention_kernel(count, chunks, scale, x_ref, wq, wk, wv, cos_ref, sin_ref, doc_c, doc_r, lab_c, lab_r, two_ref,
                     q_ref, k_ref, v_ref, o_ref, lse_ref, top_ref, g_ref, *sems):
    pos = place(count)
    greet(pos[0], count)
    gather = Gather(pos, count, chunks, two_ref, g_ref, sems)
    for c in range(chunks):
        gather.begin(c)
    gather.place_own()
    length, width = q_ref.shape
    heads = width // HD
    top_ref[...] = jnp.full(top_ref.shape, MASKED, F32)
    masks = (doc_c, doc_r, lab_c, lab_r)

    def project(h, target, weight):
        cols = slice(h * HD, (h + 1) * HD)
        raw = mm(x_ref[...], weight[:, cols])
        target[:, cols] = turn(raw, cos_ref[...], sin_ref[...]).astype(BF)

    def value():
        v_ref[...] = mm(x_ref[...], wv[...]).astype(BF)

    units = [value]
    units += [partial(project, h, *pair) for pair in ((q_ref, wq), (k_ref, wk)) for h in range(heads)]
    units += [
        partial(attention_rows, h, r0, scale, length, q_ref, k_ref, v_ref, o_ref, lse_ref, top_ref, masks)
        for h in range(heads)
        for r0 in range(0, length, QB)
    ]
    steps = [partial(gather.step, n, part, 4) for n in range(1, NZ) for part in range(4)]
    for n, unit in enumerate(units):
        unit()
        for step in steps[n * len(steps) // len(units) : (n + 1) * len(steps) // len(units)]:
            step()
    for zs in range(NZ):
        gather.got_side(zs)
    gather.drain()


def middle_kernel(count, g_chunks, s_chunks, hyper_ref, att_ref, wo_ref, hs_ref, wg_hbm, wu_hbm, wd_hbm, two_hbm,
                  b1_ref, n_ref, i_ref, x2_ref, hid_ref, dg_ref, du_ref,
                  wg, wu, wd, two, load, dhid, h_ref, x_ref, *rest):
    pos = place(count)
    loads = [
        pltpu.make_async_copy(src, dst, load.at[n])
        for n, (src, dst) in enumerate(((wd_hbm, wd), (two_hbm, two), (wg_hbm, wg), (wu_hbm, wu)))
    ]
    for copy in loads:
        copy.start()
    greet(pos[0], count)

    def part(rows, block):
        return mm(att_ref[rows, :], block_columns(wo_ref, slice(None), block, count))

    scatter = Scatter(pos, count, s_chunks, part, b1_ref, rest[:13])
    scatter.run()
    h_ref[...] = hs_ref[...] + joint(hyper_ref) * b1_ref[...]
    totals = Totals(pos, count, *rest[13:17])
    normalize(pos, count, h_ref, n_ref, i_ref, x_ref, totals)
    gather = Gather(pos, count, g_chunks, x_ref, x2_ref, rest[17:])
    for c in range(g_chunks):
        gather.begin(c)
    gather.place_own()
    tokens, width = hid_ref.shape
    tile = 256
    half = tokens // 2
    steps = width // tile

    def where(n):
        rows = pl.ds(pl.multiple_of((n // steps) * half, half), half)
        cols = pl.ds(pl.multiple_of((n % steps) * tile, tile), tile)
        return rows, cols

    def down_back(n, carry):
        rows, cols = where(n)
        dhid[rows, cols] = mm_t(two[rows, :], wd[cols, :])
        return carry

    loads[0].wait()
    loads[1].wait()
    gather.step(1)
    lax.fori_loop(0, steps, down_back, 0)
    gather.step(2)
    lax.fori_loop(steps, 2 * steps, down_back, 0)
    gather.step(3)
    for zs in range(NZ):
        gather.got_side(zs)
    loads[2].wait()
    loads[3].wait()

    def feed(n, carry):
        rows, cols = where(n)
        gate = mm(x2_ref[rows, :], wg[:, cols])
        up = mm(x2_ref[rows, :], wu[:, cols])
        sg = 1.0 / (1.0 + jnp.exp(-gate))
        back = dhid[rows, cols]
        swish = gate * sg
        hid_ref[rows, cols] = (swish * up).astype(BF)
        dg_ref[rows, cols] = (back * up * sg * (1.0 + gate * (1.0 - sg))).astype(BF)
        du_ref[rows, cols] = (back * swish).astype(BF)
        return carry

    lax.fori_loop(0, 2 * steps, feed, 0)
    scatter.drain()
    gather.drain()


def second_kernel(count, groups, g_chunks, s_chunks, hyper_ref, dg_ref, du_ref, wg, wu, n_ref, i_ref, cd_ref, x2_ref,
                  d2_ref, one_ref, gg_ref, gu_ref, sum_ref, x_ref, *rest):
    pos = place(count)
    reduce = Reduce(groups, 0, x2_ref, (dg_ref, du_ref), (gg_ref, gu_ref), rest[:9])
    rest = rest[9:]
    greet(pos[0], count, reduce)

    def part(rows, block):
        return mm_t(dg_ref[rows, :], block_rows(wg, block, count)) + mm_t(
            du_ref[rows, :], block_rows(wu, block, count)
        )

    work = reduce.work()
    now, later = work[: groups // 2 + 1], work[groups // 2 + 1 :]
    scatter = Scatter(pos, count, s_chunks, part, sum_ref, rest[:13])
    scatter.run(now)
    totals = Totals(pos, count, *rest[13:17])
    denormalize(pos, count, sum_ref, n_ref, i_ref, d2_ref, totals)
    x_ref[...] = (cd_ref[...] + joint(hyper_ref) * d2_ref[...]).astype(BF)
    gather = Gather(pos, count, g_chunks, x_ref, one_ref, rest[17:])
    for c in range(g_chunks):
        gather.begin(c)
    gather.place_own()
    gather.step(1)
    for item in later:
        item()
    gather.step(2)
    gather.step(3)
    reduce.finish()
    for zs in range(NZ):
        gather.got_side(zs)
    scatter.drain()
    gather.drain()


def back_rows(h, r0, scale, length, q_ref, k_ref, v_ref, do_ref, lse_ref, dq_acc, dk_acc, dv_acc, masks):
    cols = slice(h * HD, (h + 1) * HD)
    rows = slice(r0, r0 + QB)
    low, high = key_range(r0, length)
    doc_c, doc_r, lab_c, lab_r = masks
    q, k, v, do = q_ref[rows, cols], k_ref[low:high, cols], v_ref[low:high, cols], do_ref[rows, cols]
    s = mm_t(q, k) * scale
    allowed = head_mask(
        doc_c[rows, :1], doc_r[:1, low:high], lab_c[rows, :1], lab_r[:1, low:high], r0, low, QB, high - low
    )
    weights = jnp.where(allowed, jnp.exp(jnp.where(allowed, s, MASKED) - lse_ref[h, rows, :1]), 0.0)
    grad = mm_t(do, v)
    centre = jnp.sum(weights * grad, axis=1, keepdims=True)
    ds = (weights * (grad - centre)).astype(BF)
    dq_acc[rows, cols] = mm(ds, k) * scale
    dk_acc[low:high, cols] += t_mm(ds, q)
    dv_acc[low:high, cols] += t_mm(weights.astype(BF), do)


def attention_back_kernel(count, groups, s_chunks, scale, one_ref, wo_ref, q_ref, k_ref, v_ref, lse_ref, cos_ref, sin_ref,
                          doc_c, doc_r, lab_c, lab_r, hid_ref, wd_ref, two_ref,
                          dq_ref, dk_ref, dv_ref, b2_ref, gd_ref, do_ref, dq_acc, dk_acc, dv_acc, *scratch):
    pos = place(count)
    reduce = Reduce(groups, 1, hid_ref, (two_ref,), (gd_ref,), scratch[:9])
    scratch = scratch[9:]
    greet(pos[0], count, reduce)

    def part(rows, block):
        return mm(hid_ref[rows, :], block_columns(wd_ref, slice(None), block, count))

    scatter = Scatter(pos, count, s_chunks, part, b2_ref, scratch)
    scatter.begin(0)
    length, width = q_ref.shape
    heads = width // HD
    do_ref[...] = mm_t(one_ref[...], wo_ref[...]).astype(BF)
    dk_acc[...] = jnp.zeros_like(dk_acc)
    dv_acc[...] = jnp.zeros_like(dv_acc)
    masks = (doc_c, doc_r, lab_c, lab_r)
    todo = [(h, r0) for h in range(heads) for r0 in range(0, length, QB)]
    work = reduce.work()
    for n, (h, r0) in enumerate(todo):
        if n * s_chunks % len(todo) == 0 or s_chunks > len(todo):
            c = n * s_chunks // len(todo)
            if c + 1 < s_chunks:
                scatter.begin(c + 1)
            for item in work[c::s_chunks]:
                item()
            scatter.relay(c)
        back_rows(h, r0, scale, length, q_ref, k_ref, v_ref, do_ref, lse_ref, dq_acc, dk_acc, dv_acc, masks)
    for h in range(heads):
        cols = slice(h * HD, (h + 1) * HD)
        dq_ref[:, cols] = turn_back(dq_acc[:, cols], cos_ref[...], sin_ref[...]).astype(BF)
        dk_ref[:, cols] = turn_back(dk_acc[:, cols] * scale, cos_ref[...], sin_ref[...]).astype(BF)
    dv_ref[...] = dv_acc[...].astype(BF)
    for c in range(s_chunks):
        scatter.finish(c)
    reduce.finish()
    scatter.drain()


def last_kernel(count, groups, s_chunks, dq_ref, dk_ref, dv_ref, wq, wk, wv, n_ref, i_ref, x1_ref, att_ref, one_ref,
                d1_ref, gq_ref, gk_ref, gv_ref, go_ref, sum_ref, *rest):
    pos = place(count)
    reduce = Reduce(groups, 0, x1_ref, (dq_ref, dk_ref, dv_ref), (gq_ref, gk_ref, gv_ref), rest[:9])
    reduce_out = Reduce(groups, 1, att_ref, (one_ref,), (go_ref,), rest[9:18])
    rest = rest[18:]
    greet(pos[0], count, reduce)

    def part(rows, block):
        return (
            mm_t(dq_ref[rows, :], block_rows(wq, block, count))
            + mm_t(dk_ref[rows, :], block_rows(wk, block, count))
            + mm_t(dv_ref[rows, :], block_rows(wv, block, count))
        )

    work, work_out = reduce.work(), reduce_out.work()
    scatter = Scatter(pos, count, s_chunks, part, sum_ref, rest[:13])
    scatter.run(work[: groups // 2] + work_out[: groups // 2] + work[groups // 2 :] + work_out[groups // 2 :])
    totals = Totals(pos, count, *rest[13:])
    denormalize(pos, count, sum_ref, n_ref, i_ref, d1_ref, totals)
    reduce.finish()
    reduce_out.finish()
    scatter.drain()


VM = pl.BlockSpec(memory_space=pltpu.VMEM)
SM = pl.BlockSpec(memory_space=pltpu.SMEM)
ANY = pl.BlockSpec(memory_space=pl.ANY)


def call(kernel, ident, outs, ins, scratch, name, specs=None):
    return pl.pallas_call(
        kernel,
        out_shape=outs,
        in_specs=specs or [VM] * len(ins),
        out_specs=tuple(VM for _ in outs) if isinstance(outs, tuple) else VM,
        scratch_shapes=scratch,
        compiler_params=pltpu.CompilerParams(
            collective_id=ident, has_side_effects=True, vmem_limit_bytes=63 * 1024 * 1024
        ),
        name=name,
        cost_estimate=pl.CostEstimate(flops=50_000_000_000, bytes_accessed=8_000_000, transcendentals=0),
    )(*ins)


def shape(dtype, *dims):
    return jax.ShapeDtypeStruct(dims, dtype)


AG_CHUNKS = 8
RS_CHUNKS = 4
ROWS = 128


def rows_call(kernel, hyper, ins, outs, name):
    tokens = ins[0].shape[-2]

    def spec(a):
        if a.shape[-2] != tokens:
            return pl.BlockSpec(a.shape, lambda t: (0,) * len(a.shape))
        if len(a.shape) == 3:
            return pl.BlockSpec((a.shape[0], ROWS, a.shape[2]), lambda t: (0, t, 0))
        return pl.BlockSpec((ROWS, a.shape[1]), lambda t: (t, 0))

    return pl.pallas_call(
        kernel,
        grid=(tokens // ROWS,),
        out_shape=outs,
        in_specs=[SM] + [spec(a) for a in ins],
        out_specs=tuple(spec(a) for a in outs),
        compiler_params=pltpu.CompilerParams(vmem_limit_bytes=60 * 1024 * 1024),
        name=name,
        cost_estimate=pl.CostEstimate(flops=1_000_000_000, bytes_accessed=20_000_000, transcendentals=0),
    )(hyper, *ins)


def hyper_grad(hyper, v):
    pre1, post0, mix0, mix1 = hyper[1, :, 0], hyper[0, :, 1], hyper[0, :, 2:], hyper[1, :, 2:]
    cs, cb1, cb2, d2s, d1s, d2b1 = v[:16].reshape(4, 4), v[16:20], v[20:24], v[24:28], v[28:32], v[32]
    flat = partial(jnp.sum, axis=-1)
    g1_pre = flat(mix0 * d2s[None, :]) + post0 * d2b1
    g1_mix = jnp.sum(cs[:, None, :] * mix0[None, :, :], axis=2) + cb1[:, None] * post0[None, :]
    g0_post = jnp.sum(mix1 * cb1[:, None], axis=0) + pre1 * d2b1
    g0_mix = jnp.sum(mix1[:, :, None] * cs[:, None, :], axis=0) + pre1[:, None] * d2s[None, :]
    return jnp.stack([hyper_rows(d1s, g0_post, g0_mix), hyper_rows(g1_pre, cb2, g1_mix)])


def per_device(
    streams,
    cotangent,
    w_query,
    w_key,
    w_value,
    w_out,
    w_gate,
    w_up,
    w_down,
    hyper,
    doc_ids,
    span_starts,
    span_lengths,
):
    length = doc_ids.shape[1]
    tokens, bw = streams.shape[1:]
    count, groups = lax.axis_size("wide"), lax.axis_size("dp")
    heads = bw // HD
    scale = 1.0 / math.sqrt(HD)
    cos, sin = rope_tables(length, HD)
    labels = span_labels(jnp.arange(length, dtype=jnp.int32), span_starts[0], span_lengths[0])
    doc_r = jnp.broadcast_to(doc_ids, (8, length))
    lab_r = jnp.broadcast_to(labels[None, :], (8, length))
    doc_c = jnp.broadcast_to(doc_ids[0][:, None], (length, 128))
    lab_c = jnp.broadcast_to(labels[:, None], (length, 128))
    masks = [doc_c, doc_r, lab_c, lab_r]
    gate_w, up_w, down_w = (
        lax.all_gather(w_gate, "dp", axis=0, tiled=True),
        lax.all_gather(w_up, "dp", axis=0, tiled=True),
        lax.all_gather(w_down, "dp", axis=1, tiled=True),
    )
    hidden_units = gate_w.shape[1]
    small = shape(F32, tokens, bw)
    low = shape(BF, tokens, bw)
    whole = shape(BF, tokens, count * bw)
    stat = shape(F32, tokens, 128)
    wide_low = shape(BF, tokens, hidden_units)
    v = pltpu.VMEM
    scatter_scratch = Scatter.scratch(count, RS_CHUNKS, tokens, bw)
    gather_scratch = Gather.scratch(count, AG_CHUNKS)
    total_scratch = Totals.scratch(count, tokens)

    h_one, h_streams, cot_one, two_part, sums_a = rows_call(
        enter_kernel, hyper, [streams, cotangent], (small, small, small, low, shape(F32, 16, 8, 128)), "enter"
    )
    tall = shape(BF, count * bw, bw)
    x_one, kept_one, inverse_one, query_w, key_w, value_w, out_w = call(
        partial(first_kernel, count, groups, AG_CHUNKS),
        0,
        (whole, small, stat, tall, tall, tall, shape(BF, bw, count * bw)),
        [h_one, w_query, w_key, w_value, w_out],
        [v((tokens, bw), BF)] + Spread.scratch(groups, 4) + total_scratch + gather_scratch,
        "first",
    )
    queries, keys, values, attended, log_sums, tops, two_grad = call(
        partial(attention_kernel, count, AG_CHUNKS, scale),
        1,
        (low, low, low, low, shape(F32, heads, tokens, 128), shape(F32, 8, 128), whole),
        [x_one, query_w, key_w, value_w, cos, sin] + masks + [two_part],
        gather_scratch,
        "attention",
    )
    branch_one, kept_two, inverse_two, x_two, hidden, gate_grad, up_grad = call(
        partial(middle_kernel, count, AG_CHUNKS, RS_CHUNKS),
        2,
        (small, small, stat, whole, wide_low, wide_low, wide_low),
        [hyper, attended, out_w, h_streams, gate_w, up_w, down_w, two_grad],
        [
            v(gate_w.shape, BF),
            v(up_w.shape, BF),
            v(down_w.shape, BF),
            v((tokens, count * bw), BF),
            dma(4),
            v((tokens, hidden_units), F32),
            v((tokens, bw), F32),
            v((tokens, bw), BF),
        ]
        + scatter_scratch
        + total_scratch
        + gather_scratch,
        "middle",
        [SM, VM, VM, VM, ANY, ANY, ANY, ANY],
    )
    wide_grad = shape(F32, *w_gate.shape)
    h_two_grad, one_grad, gate_shard, up_shard = call(
        partial(second_kernel, count, groups, AG_CHUNKS, RS_CHUNKS),
        3,
        (small, whole, wide_grad, wide_grad),
        [hyper, gate_grad, up_grad, gate_w, up_w, kept_two, inverse_two, cot_one, x_two],
        [v((tokens, bw), F32), v((tokens, bw), BF)]
        + Reduce.scratch(groups, 0, x_two, (w_gate, w_up))
        + scatter_scratch
        + total_scratch
        + gather_scratch,
        "second",
        [SM] + [VM] * 8,
    )
    query_low, key_low, value_low, branch_two, down_shard = call(
        partial(attention_back_kernel, count, groups, RS_CHUNKS, scale),
        4,
        (low, low, low, small, shape(F32, *w_down.shape)),
        [one_grad, out_w, queries, keys, values, log_sums, cos, sin] + masks + [hidden, down_w, two_grad],
        [v((tokens, bw), BF)] + [v((tokens, bw), F32)] * 3 + Reduce.scratch(groups, 1, hidden, (w_down,)) + scatter_scratch,
        "attention_back",
    )
    narrow_grad = shape(F32, *w_query.shape)
    h_one_grad, query_shard, key_shard, value_shard, out_shard = call(
        partial(last_kernel, count, groups, RS_CHUNKS),
        5,
        (small, narrow_grad, narrow_grad, narrow_grad, shape(F32, *w_out.shape)),
        [query_low, key_low, value_low, query_w, key_w, value_w, kept_one, inverse_one, x_one, attended, one_grad],
        [v((tokens, bw), F32)]
        + Reduce.scratch(groups, 0, x_one, (w_query, w_key, w_value))
        + Reduce.scratch(groups, 1, attended, (w_out,))
        + scatter_scratch
        + total_scratch,
        "last",
    )
    streams_shape = shape(F32, 4, tokens, bw)
    out_streams, streams_grad, sums_b = rows_call(
        leave_kernel,
        hyper,
        [streams, cotangent, branch_one, branch_two, h_two_grad, h_one_grad],
        (streams_shape, streams_shape, shape(F32, 17, 8, 128)),
        "leave",
    )
    sums, best = call(
        partial(total_kernel, count, groups),
        6,
        (shape(F32, 40, 128), shape(F32, 8, 128)),
        [sums_a, sums_b, tops],
        [
            v((40, 128), F32),
            v((groups - 1, 40, 128), F32),
            v((count - 1, 40, 128), F32),
            v((8, 128), F32),
            v((groups - 1, 8, 128), F32),
            dma(groups - 1),
            dma(groups - 1),
            dma(count - 1),
            dma(count - 1),
            dma(groups - 1),
            dma(groups - 1),
        ],
        "totals",
    )
    head_top = best[:heads, 0]
    clip_scale = jnp.sqrt(CLIP_TAU / jnp.maximum(head_top, CLIP_TAU))
    columns = jnp.repeat(clip_scale, HD)[None, :]
    return (
        out_streams,
        streams_grad,
        query_shard,
        key_shard,
        value_shard,
        out_shard,
        gate_shard,
        up_shard,
        down_shard,
        hyper_grad(hyper, sums[:, 0]),
        clip_scale,
        w_query.astype(F32) * columns,
        w_key.astype(F32) * columns,
    )


def solution(mesh):
    return jax.shard_map(
        per_device,
        mesh=mesh,
        in_specs=(
            P(None, "dp", "wide"),
            P(None, "dp", "wide"),
            P("dp", "wide"),
            P("dp", "wide"),
            P("dp", "wide"),
            P("wide", "dp"),
            P("dp", "wide"),
            P("dp", "wide"),
            P("wide", "dp"),
            P(),
            P("dp", None),
            P("dp", None),
            P("dp", None),
        ),
        out_specs=(
            P(None, "dp", "wide"),
            P(None, "dp", "wide"),
            P("dp", "wide"),
            P("dp", "wide"),
            P("dp", "wide"),
            P("wide", "dp"),
            P("dp", "wide"),
            P("dp", "wide"),
            P("wide", "dp"),
            P(),
            P("wide"),
            P("dp", "wide"),
            P("dp", "wide"),
        ),
        check_vma=False,
    )
```
